256 devices in a mesh: lon: 16 (over z, x_hi), lat: 4 (over y), mem: 4 (over x_lo, core).
Axes of the slice: x: 4 (x_hi: 2, x_lo: 2; x = x_hi * 2 + x_lo), y: 4, z: 8, core: 2. Of those that a mesh axis runs over, the one named last changes fastest.
Arguments:
- anomalies: bfloat16 [32, 4, 1024, 512], P('mem', None, 'lon', 'lat'), may hold values from -6 to 6
- spread: float32 [4, 1024, 512], P(None, 'lon', 'lat'), may hold values from 0.5 to 2
- obs_index: int32 [16, 4, 2048], P('lon', 'lat'), may hold values from 0 to 32767
- innovation: float32 [16, 4, 2048], P('lon', 'lat'), may hold values from -6 to 6
- obs_weight: float32 [16, 4, 2048], P('lon', 'lat'), may hold values from 0.5 to 8
- band_width: int32 [2, 4], replicated, may hold values from 6 to 12, as said below
Outputs:
- control_ens: float32 [32, 4, 1024, 512], P('mem', None, 'lon', 'lat')
- control_static: float32 [4, 1024, 512], P(None, 'lon', 'lat')
The draws below stay inside these ranges and needn't reach their ends.
Inputs may be any that keep to these rules, and one draw needn't show every extreme that they name: `obs_index`: A cell of the tile's 4 x 64 x 128 block, flattened with latitude fastest. `band_width`: in each of the two rows some level has exactly 12.
All inputs are finite; a program needn't handle non-finite values.
Results may differ from the reference program's by a relative error of at most 0.0003.
Values may be sent and summed in bfloat16 or wider, within the bound.
A program may use at most 64 MiB of HBM per device.

```python
import math
import jax
import jax.numpy as jnp
from jax import lax

LON_DEV = 64
LAT_DEV = 128
LEVELS = 4
OBS_DEV = 2048
BAND = 12
ITERS = 2
MEMBERS = 32
NLON = 1024
NLAT = 512
N_LON = 16
N_LAT = 4


def draw_band_width(key, part):
    lower = jax.random.randint(jax.random.fold_in(key, 11), (2, LEVELS), BAND // 2, BAND + 1)
    widest = jax.random.randint(jax.random.fold_in(key, 12), (2, 1), 0, LEVELS)
    level_iota = jnp.arange(LEVELS, dtype=jnp.int32)[None, :]
    return jnp.where(level_iota == widest, BAND, lower).astype(jnp.int32)


def with_ends(values, rng, least, largest):
    shape = values.shape
    index_at = [jax.random.randint(jax.random.fold_in(rng, axis), (), 0, shape[axis]) for axis in range(len(shape))]
    values = values.at[tuple(index_at)].set(least)
    longest = shape.index(max(shape))
    index_at[longest] = (index_at[longest] + 1) % shape[longest]
    return values.at[tuple(index_at)].set(largest)


def shard_levels(stream_key, dims, pieces, smallest, high):
    def one(position, blocks):
        draws = jax.random.uniform(jax.random.fold_in(jax.random.fold_in(stream_key, 6), position), (blocks,), jnp.float32, smallest / len(pieces), high / len(pieces))
        return jnp.repeat(jnp.exp(draws), dims[position] // blocks).reshape((-1,) + (1,) * (len(dims) - position - 1))

    loudness = one(*pieces[0])
    for cut in pieces[1:]:
        loudness = loudness * one(*cut)
    return loudness


def noise(key, dims, scale, reach, split=(), held_as=jnp.bfloat16):
    drawn = jax.random.normal(key, dims, jnp.float32) * scale
    if len(split) > 0:
        drawn = shard_levels(key, dims, split, -0.22, 0.18) * drawn
    return jnp.clip(drawn, min=-reach, max=reach).astype(held_as)


def setup_inputs(seed: int = 0) -> dict:
    streams_of = jax.random.split(jax.random.key(seed), 7)
    return {
        "anomalies": noise(streams_of[0], (MEMBERS, LEVELS, NLON, NLAT), 1.0, 6.0, ((0, 4), (2, 16), (3, 4))),
        "spread": jnp.clip(jnp.exp(math.log(2.0) - 1.3862944 * jax.random.uniform(streams_of[1], (LEVELS, NLON, NLAT), jnp.float32) ** shard_levels(streams_of[1], (LEVELS, NLON, NLAT), ((1, 16), (2, 4)), -0.2, 0.2)), 0.5, 2.0),
        "obs_index": with_ends(jax.random.randint(streams_of[2], (N_LON, N_LAT, OBS_DEV), 0, LEVELS * LON_DEV * LAT_DEV), jax.random.fold_in(streams_of[2], 1), 0, (LEVELS * LON_DEV * LAT_DEV) - 1).astype(jnp.int32),
        "innovation": noise(streams_of[3], (N_LON, N_LAT, OBS_DEV), 1.0, 6.0, ((0, 16), (1, 4)), jnp.float32),
        "obs_weight": jnp.clip(jnp.exp(math.log(8.0) - 2.7725887 * jax.random.uniform(streams_of[4], (N_LON, N_LAT, OBS_DEV), jnp.float32) ** shard_levels(streams_of[4], (N_LON, N_LAT, OBS_DEV), ((0, 16), (1, 4)), -0.2, 0.2)), 0.5, 8.0),
        "band_width": draw_band_width(jax.random.fold_in(streams_of[6], 71), 0),
    }


hybrid_ens = 0.75
hybrid_static = 0.25

def band_table(band_width):
    offsets = jnp.arange(-BAND, BAND + 1).astype(jnp.float32)
    widths = band_width.astype(jnp.float32)[..., None]
    shape_raw = jnp.exp(-0.5 * (offsets / (0.5 * widths)) ** 2)
    shape_raw = jnp.where(jnp.abs(offsets) <= widths, shape_raw, 0.0)
    return shape_raw / lax.optimization_barrier(jnp.sum(shape_raw, axis=-1, keepdims=True))

def localize(field, weights_lon, weights_lat):
    lon_smooth = jnp.zeros_like(field)
    for shift in range(2 * BAND + 1):
        lon_smooth = lon_smooth + weights_lon[:, shift][:, None, None] * jnp.roll(field, BAND - shift, axis=1)
    padded = jnp.pad(lon_smooth, ((0, 0), (0, 0), (BAND, BAND)))
    result = jnp.zeros_like(field)
    for shift in range(2 * BAND + 1):
        result = result + weights_lat[:, shift][:, None, None] * padded[:, :, shift:shift + NLAT]
    return result

def reference(anomalies, spread, obs_index, innovation, obs_weight, band_width):
    band_weights = band_table(band_width)
    coef_ens = math.sqrt(hybrid_ens / MEMBERS)
    coef_static = math.sqrt(hybrid_static)

    def smooth(fields):
        return lax.map(lambda member_field: localize(member_field, band_weights[0], band_weights[1]), fields)
    plane_cells = LON_DEV * LAT_DEV
    obs_level = obs_index // plane_cells
    in_plane = obs_index % plane_cells
    tile_lon = jnp.arange(N_LON, dtype=jnp.int32)[:, None, None]
    tile_lat = jnp.arange(N_LAT, dtype=jnp.int32)[None, :, None]
    flat_index = ((obs_level * NLON + tile_lon * LON_DEV + in_plane // LAT_DEV) * NLAT + tile_lat * LAT_DEV + in_plane % LAT_DEV).reshape(-1).astype(jnp.int32)
    weights = obs_weight.reshape(-1)
    values = innovation.reshape(-1)
    cell_count = LEVELS * NLON * NLAT

    def scatter(obs_term):
        return jnp.zeros((cell_count,), jnp.float32).at[flat_index].add(obs_term).reshape(LEVELS, NLON, NLAT)

    def adjoint(gradient):
        products = jnp.concatenate([coef_ens * anomalies.astype(jnp.float32) * gradient[None], (coef_static * spread * gradient)[None]], axis=0)
        return smooth(products)

    def hessian(direction):
        localized = smooth(direction)
        combined = coef_ens * lax.optimization_barrier(jnp.sum(anomalies.astype(jnp.float32) * localized[:MEMBERS], axis=0)) + coef_static * spread * localized[MEMBERS]
        gradient = scatter(weights * combined.reshape(-1)[flat_index])
        return direction + adjoint(gradient)
    right_side = adjoint(scatter(weights * values))
    control = jnp.zeros_like(right_side)
    residual = right_side
    direction = right_side
    norm_now = jnp.sum(residual * residual)
    for iteration in range(ITERS):
        hess_image = hessian(direction)
        step_size = norm_now / jnp.sum(direction * hess_image)
        control = control + step_size * direction
        residual = residual - step_size * hess_image
        norm_next = jnp.sum(residual * residual)
        direction = residual + norm_next / norm_now * direction
        norm_now = norm_next
    return (control[:MEMBERS], control[MEMBERS])
```

```python
import math

import jax
import jax.numpy as jnp
from jax import lax
from jax.sharding import PartitionSpec as P

BAND = 12
HALO = 2 * BAND
hybrid_ens = 0.75
hybrid_static = 0.25
HI = lax.Precision.HIGHEST


def with_halo(block, axis, dim, width):
    count = lax.axis_size(axis)
    forward = [(i, (i + 1) % count) for i in range(count)]
    backward = [(target, source) for source, target in forward]
    low = lax.ppermute(lax.slice_in_dim(block, block.shape[dim] - width, None, axis=dim), axis, forward)
    high = lax.ppermute(lax.slice_in_dim(block, 0, width, axis=dim), axis, backward)
    return jnp.concatenate([low, block, high], axis=dim)


def band_table(band_width):
    offsets = jnp.arange(-BAND, BAND + 1).astype(jnp.float32)
    widths = band_width.astype(jnp.float32)[..., None]
    shape_raw = jnp.exp(-0.5 * (offsets / (0.5 * widths)) ** 2)
    shape_raw = jnp.where(jnp.abs(offsets) <= widths, shape_raw, 0.0)
    return shape_raw / jnp.sum(shape_raw, axis=-1, keepdims=True)


def band_matrix(weights, rows, cols, shift):
    diff = jnp.arange(cols)[None, :] - jnp.arange(rows)[:, None] - shift + BAND
    onehot = (diff[:, :, None] == jnp.arange(2 * BAND + 1)).astype(jnp.float32)
    return jnp.einsum("ls,ijs->lij", weights, onehot, precision=HI)


def per_device(anomalies, spread, obs_index, innovation, obs_weight, band_width):
    members = anomalies.shape[0]
    levels, lon_cells, lat_cells = spread.shape
    mem_count = lax.axis_size("mem")
    coef_ens = math.sqrt(hybrid_ens / (members * mem_count))
    coef_static = math.sqrt(hybrid_static)
    table = band_table(band_width)
    lat_index = lax.axis_index("lat")
    inside_low = (lat_index > 0)
    inside_high = (lat_index < lax.axis_size("lat") - 1)

    def inside(cells, width):
        at = jnp.arange(cells) - width
        return ((at >= 0) | inside_low) & ((at < lat_cells) | inside_high)

    lon1 = band_matrix(table[0], lon_cells, lon_cells + HALO, BAND)
    lon2 = jnp.einsum("lij,ljk->lik", lon1, band_matrix(table[0], lon_cells + HALO, lon_cells + 2 * HALO, BAND), precision=HI)
    lat1 = band_matrix(table[1], lat_cells, lat_cells + HALO, BAND) * inside(lat_cells + HALO, BAND)
    lat2 = jnp.einsum("lij,ljk->lik", lat1, band_matrix(table[1], lat_cells + HALO, lat_cells + 2 * HALO, BAND), precision=HI) * inside(lat_cells + 2 * HALO, HALO)

    obs_flat = obs_index.reshape(-1)
    weights = obs_weight.reshape(-1)
    both = jnp.stack([weights, weights * innovation.reshape(-1)], axis=1)
    fields = jnp.zeros((levels * lon_cells * lat_cells, 2), jnp.float32).at[obs_flat].add(both)
    obs_diag = fields[:, 0].reshape(spread.shape)
    t0 = fields[:, 1].reshape(spread.shape)

    def extended(field):
        lead = field.ndim - 2
        return with_halo(with_halo(field, "lat", lead + 1, HALO), "lon", lead, HALO)

    ens = extended(anomalies)
    stat = extended(spread)
    owner = jnp.where(lax.axis_index("mem") == 0, 1.0, 0.0).astype(jnp.float32)

    def smooth(fields, lon_matrix, lat_matrix):
        half = jnp.einsum("flja,lka->fljk", fields, lat_matrix, precision=HI)
        return jnp.einsum("flja,lij->flia", half, lon_matrix, precision=HI)

    def joined(z_ext):
        return jnp.concatenate([coef_ens * ens.astype(jnp.float32) * z_ext, (coef_static * stat * z_ext)[None]], axis=0)

    def covariance(z_ext):
        local = smooth(joined(z_ext), lon2, lat2)
        part = coef_ens * jnp.sum(anomalies.astype(jnp.float32) * local[:members], axis=0) + owner * coef_static * spread * local[members]
        copies = jnp.broadcast_to(part, (mem_count, *part.shape))
        return lax.all_to_all(copies, "mem", split_axis=0, concat_axis=0, tiled=True).sum(axis=0)

    t0_ext = extended(t0)
    y0 = covariance(t0_ext)
    t1 = obs_diag * y0
    t1_ext = extended(t1)
    y1 = covariance(t1_ext)
    sums = jnp.stack([jnp.sum(t0 * y0), jnp.sum(t1 * y0), jnp.sum(t1 * y1), jnp.sum(y1 * obs_diag * y1)])
    sums = lax.psum(sums, ("lon", "lat", "mem"))
    u, v, s = sums[1] / sums[0], sums[2] / sums[0], sums[3] / sums[0]
    alpha = 1.0 / (1.0 + u)
    beta = (v - u * u) * alpha * alpha
    g, h = 1.0 - alpha + beta, -alpha
    alpha_next = beta / (g * g * (1.0 + u) + 2.0 * g * h * (u + v) + h * h * (v + s))
    control = joined((alpha + alpha_next * g) * t0_ext + alpha_next * h * t1_ext)[:, :, BAND:-BAND, BAND:-BAND]
    control = smooth(control, lon1, lat1)
    return control[:members], control[members]


def solution(mesh):
    return jax.shard_map(
        per_device,
        mesh=mesh,
        in_specs=(
            P("mem", None, "lon", "lat"),
            P(None, "lon", "lat"),
            P("lon", "lat", None),
            P("lon", "lat", None),
            P("lon", "lat", None),
            P(),
        ),
        out_specs=(P("mem", None, "lon", "lat"), P(None, "lon", "lat")),
        check_vma=False,
    )
```

```python
import math

import jax
import jax.numpy as jnp
from jax import lax
from jax.experimental import pallas as pl
from jax.experimental.pallas import tpu as pltpu
from jax.sharding import PartitionSpec as P

BAND = 12
HALO = 2 * BAND
PAD = 32
hybrid_ens = 0.75
hybrid_static = 0.25
F32, BF16 = jnp.float32, jnp.bfloat16
HI = lax.Precision.HIGHEST
MESH = pl.DeviceIdType.MESH
AROUND = [(dx, dy) for dy in (0, 1, -1) for dx in (1, -1, 0) if (dx, dy) != (0, 0)]


def iota(shape, axis):
    return lax.broadcasted_iota(jnp.int32, shape, axis)


def dot(a, b, precision=None):
    return jnp.dot(a, b, preferred_element_type=F32, precision=precision)


def split(x):
    high = x.astype(BF16)
    return high, (x - high.astype(F32)).astype(BF16)


def kernel(dims, band_ref, a_ref, s_ref, idx_ref, inn_ref, wt_ref, p_ref, ps_ref, lam_ref,
           ac, kl, kr, hl, hr, f0c, k0l, k0r, f0l, f0r, f1c, k1l, k1r, f1l, f1r,
           obs, mlat, nlon, xs, ub, sb, y_ref, yr, t1_ref, gather_mem, gather_lat, gather_lon,
           a_send, a_recv, f0_send, f0_recv, f1_send, f1_recv, r0_send, r0_recv, r1_send, r1_recv,
           g_send, g_recv, q_send, q_recv, sm_send, sm_recv, sa_send, sa_recv, so_send, so_recv):
    n_lon, n_lat, n_mem, members, levels, rows, cols = dims
    lon, lat, mem = lax.axis_index("lon"), lax.axis_index("lat"), lax.axis_index("mem")
    ce2 = hybrid_ens / (members * n_mem)
    cs2 = hybrid_static
    ext = rows + 2 * PAD

    def at(dlon=0, dlat=0, dmem=0):
        return {
            "lon": lax.rem(lon + (dlon + n_lon), n_lon),
            "lat": lax.rem(lat + (dlat + n_lat), n_lat),
            "mem": lax.rem(mem + (dmem + n_mem), n_mem),
        }

    def copy(src, dst, send, recv, device):
        return pltpu.make_async_remote_copy(
            src_ref=src, dst_ref=dst, send_sem=send, recv_sem=recv, device_id=device, device_id_type=MESH
        )

    partners = [(dx, dy, 0) for dx, dy in AROUND]
    partners += [(0, 0, o) for o in range(1, n_mem)]
    partners += [(0, o, 0) for o in range(2, n_lat - 1)]
    partners += [(o, 0, 0) for o in range(2, n_lon - 1)]
    barrier = pltpu.get_barrier_semaphore()
    for partner in partners:
        pl.semaphore_signal(barrier, inc=1, device_id=at(*partner), device_id_type=MESH)

    own = pl.ds(PAD, rows)
    low, high = pl.ds(PAD - HALO, HALO), pl.ds(PAD + rows, HALO)
    first, last = pl.ds(0, HALO), pl.ds(rows - HALO, HALO)

    sel_row, sel_col = iota((levels * cols, 2 * cols), 0), iota((levels * cols, 2 * cols), 1)
    sel_level, sel_lat = sel_row // cols, lax.rem(sel_row, cols)
    spot = lax.rem(sel_col, cols) - HALO * sel_level
    wanted = jnp.where(sel_col < cols, spot + (cols - HALO), spot)
    select = jnp.where((spot >= 0) & (spot < HALO) & (sel_lat == wanted), 1.0, 0.0)

    packed = dot(
        jnp.concatenate([a_ref[:, l].reshape(members * rows, cols) for l in range(levels)], axis=1),
        select.astype(BF16),
    ).astype(BF16)
    kl[...] = packed[:, :cols].reshape(members, rows, cols)
    kr[...] = packed[:, cols:].reshape(members, rows, cols)
    edges = (pl.ds(0, PAD - HALO), pl.ds(PAD + rows + HALO, PAD - HALO))
    for edge in edges:
        ac[:, :, edge, :] = jnp.zeros((members, levels, PAD - HALO, cols), BF16)
        for ref in (hl, hr):
            ref[:, edge, :] = jnp.zeros((members, PAD - HALO, cols), BF16)
        for ref in (f0c, f0l, f0r, f1c, f1l, f1r):
            ref[:, edge, :] = jnp.zeros((ref.shape[0], PAD - HALO, cols), F32)
    ac[:, :, own, :] = a_ref[...]
    f0c[levels, own, :] = s_ref[mem]

    r, c = iota((cols, cols), 0), iota((cols, cols), 1)
    inside_low = jnp.where(lat > 0, 1.0, 0.0).astype(F32)
    inside_high = jnp.where(lat < n_lat - 1, 1.0, 0.0).astype(F32)
    offsets = iota((8, cols), 1) - BAND

    def level_matrices(l, carry):
        def band_of(which):
            width = jnp.full((1, 1), band_ref[which, l].astype(F32), F32)

            def raw(diff):
                d = diff.astype(F32)
                ratio = d / (0.5 * width)
                return jnp.where(jnp.abs(d) <= width, jnp.exp(-0.5 * (ratio * ratio)), 0.0)

            total = jnp.sum(raw(offsets), axis=1, keepdims=True)[0:1]
            return lambda diff: raw(diff) / total

        band = band_of(1)
        spot = r - HALO * l
        valid = jnp.where((spot >= 0) & (spot < HALO), 1.0, 0.0)
        d0, dm, dp = band(r - c), band(r - cols - c), band(r + cols - c)
        from_low = spot + (cols - HALO)
        dml, d0l = band(from_low - cols - c) * valid, band(from_low - c) * valid
        dpr, d0r = band(spot + cols - c) * valid, band(spot - c) * valid
        twice = [
            dot(d0, d0, HI) + inside_low * dot(dp, dm, HI) + inside_high * dot(dm, dp, HI),
            inside_low * (dot(d0l, dm, HI) + dot(dml, d0, HI)),
            inside_high * (dot(d0r, dp, HI) + dot(dpr, d0, HI)),
        ]
        once = [d0, inside_low * dml, inside_high * dpr]
        for part in range(3):
            hi, lo = split(jnp.concatenate([twice[part], once[part]], axis=1))
            mlat[l, part * cols:(part + 1) * cols, :] = hi
            mlat[l, (3 + part) * cols:(4 + part) * cols, :] = hi
            mlat[l, (6 + part) * cols:(7 + part) * cols, :] = lo
        band = band_of(0)
        near = band(iota((rows, ext), 0) + PAD - iota((rows, ext), 1))
        far = band(iota((ext, ext), 0) - iota((ext, ext), 1))
        for which, matrix in enumerate((dot(near, far, HI), near)):
            hi, lo = split(matrix)
            nlon[which, l, 0:rows, :] = hi
            nlon[which, l, rows:2 * rows, :] = lo
        return carry

    lax.fori_loop(0, levels, level_matrices, 0)

    pl.semaphore_wait(barrier, len(partners))

    def halo(centre, source, left, right, packed_left, packed_right, send, recv):
        copies = []
        for number, (dx, dy) in enumerate(AROUND):
            from_rows = {1: last, -1: first, 0: pl.ds(0, rows)}[dx]
            to_rows = {1: low, -1: high, 0: own}[dx]
            if dy == 0:
                src, dst = source(dx), centre.at[..., to_rows, :] if len(centre.shape) == 3 else centre.at[:, :, to_rows, :]
            else:
                src = (packed_left if dy == 1 else packed_right).at[:, from_rows, :]
                dst = (left if dy == 1 else right).at[:, to_rows, :]
            one = copy(src, dst, send.at[number], recv.at[number], at(dx, dy))
            one.start()
            copies.append(one)
        return copies

    a_copies = halo(ac, lambda dx: a_ref.at[:, :, last if dx == 1 else first, :], hl, hr, kl, kr, a_send, a_recv)

    index = idx_ref[...]
    weight = wt_ref[...]
    at_row, at_col = index // cols, lax.rem(index, cols)
    count = index.shape[1]
    columns = jnp.where(iota((cols, count), 0) == at_col, 1.0, 0.0).astype(BF16)

    def thirds(v):
        one = v.astype(BF16).astype(F32)
        two = (v - one).astype(BF16).astype(F32)
        return [one, two, v - one - two]

    terms = thirds(weight) + thirds(weight * inn_ref[...])

    def level_fields(l, carry):
        here = (iota((rows, count), 0) + rows * l) == at_row
        stacked = jnp.concatenate([jnp.where(here, t, 0.0).astype(BF16) for t in terms], axis=0)
        sums = lax.dot_general(stacked, columns, (((1,), (1,)), ((), ())), preferred_element_type=F32)
        obs[l] = sums[0:rows] + sums[rows:2 * rows] + sums[2 * rows:3 * rows]
        f0c[l, own, :] = sums[3 * rows:4 * rows] + sums[4 * rows:5 * rows] + sums[5 * rows:]
        return carry

    lax.fori_loop(0, levels, level_fields, 0)

    def pack(centre, left, right, slot):
        both = dot(jnp.concatenate([centre[l, own, :] for l in range(levels)], axis=1), select, HI)
        left[slot] = both[:, :cols]
        right[slot] = both[:, cols:]

    pack(f0c, k0l, k0r, 0)
    spot = lax.rem(iota((cols, 2 * cols), 1), cols) - HALO * mem
    wanted = jnp.where(iota((cols, 2 * cols), 1) < cols, spot + (cols - HALO), spot)
    mine = jnp.where((spot >= 0) & (spot < HALO) & (iota((cols, 2 * cols), 0) == wanted), 1.0, 0.0)
    both = dot(s_ref[mem], mine, HI)
    k0l[1] = both[:, :cols]
    k0r[1] = both[:, cols:]
    field_rows = {1: pl.ds(PAD + rows - HALO, HALO), -1: pl.ds(PAD, HALO)}
    f0_copies = halo(f0c, lambda dx: f0c.at[:, field_rows[dx], :], f0l, f0r, k0l, k0r, f0_send, f0_recv)
    for one in a_copies + f0_copies:
        one.wait_recv()

    def lon_pass(l, u_hi, u_lo, which):
        tall = dot(nlon[which, l], u_hi)
        return tall[0:rows] + tall[rows:] + dot(nlon[which, l, 0:rows, :], u_lo)

    def apply(centre, left, right, turn):
        zl, zr = left[0], right[0]
        for k in range(members):
            spans = pl.ds(k * ext, ext)
            for part, (rim, z) in enumerate(((hl, zl), (hr, zr))):
                hi, lo = split(rim[k].astype(F32) * z)
                xs[spans, (1 + part) * cols:(2 + part) * cols] = hi
                xs[spans, (4 + part) * cols:(5 + part) * cols] = lo

        def one_level(l, carry):
            z = centre[l]
            for k in range(members):
                hi, lo = split(ac[k, l].astype(F32) * z)
                xs[pl.ds(k * ext, ext), 0:cols] = hi
                xs[pl.ds(k * ext, ext), 3 * cols:4 * cols] = lo
            ub[...] = dot(xs[...], mlat[l, 0:6 * cols, :]) + dot(xs[:, 0:3 * cols], mlat[l, 6 * cols:, :])
            total = jnp.zeros((rows, cols), F32)
            for k in range(members):
                hi, lo = split(ub[pl.ds(k * ext, ext), :])
                total += a_ref[k, l].astype(F32) * lon_pass(l, hi[:, :cols], lo[:, :cols], 0)
                p_ref[turn, k, l] = math.sqrt(ce2) * lon_pass(l, hi[:, cols:], lo[:, cols:], 1)
            y_ref[l] = ce2 * total
            return carry

        lax.fori_loop(0, levels, one_level, 0)
        his, los = [], []
        for stat, z in ((f0c[levels], centre[mem]), (f0l[1], zl), (f0r[1], zr)):
            hi, lo = split(stat * z)
            his.append(hi)
            los.append(lo)
        u = dot(jnp.concatenate(his + los, axis=1), mlat[mem, 0:6 * cols, :])
        u += dot(jnp.concatenate(his, axis=1), mlat[mem, 6 * cols:, :])
        hi, lo = split(u)
        y_ref[mem] = y_ref[mem] + cs2 * s_ref[mem] * lon_pass(mem, hi[:, :cols], lo[:, :cols], 0)
        ps_ref[turn, mem] = math.sqrt(cs2) * lon_pass(mem, hi[:, cols:], lo[:, cols:], 1)

    def reduced(slots, send, recv):
        copies = []
        for o in range(1, n_mem):
            peer = lax.rem(mem + o, n_mem)
            one = copy(y_ref.at[peer], slots.at[o - 1], send.at[o - 1], recv.at[o - 1], at(0, 0, o))
            one.start()
            copies.append(one)
        for one in copies:
            one.wait()
        return y_ref[mem] + slots[0] + slots[1] + slots[2]

    apply(f0c, f0l, f0r, 0)
    y0 = reduced(yr.at[0], r0_send, r0_recv)
    t0 = f0c[mem, own, :]
    t1 = obs[mem] * y0
    t1_ref[...] = t1
    f1c[mem, own, :] = t1
    g_copies = []
    for o in range(1, n_mem):
        one = copy(t1_ref, f1c.at[mem, own, :], g_send.at[o - 1], g_recv.at[o - 1], at(0, 0, o))
        one.start()
        g_copies.append(one)
    for one in g_copies:
        one.wait_recv()
    pack(f1c, k1l, k1r, 0)
    f1_copies = halo(f1c, lambda dx: f1c.at[:, field_rows[dx], :], f1l, f1r, k1l, k1r, f1_send, f1_recv)
    for one in f1_copies:
        one.wait_recv()
    apply(f1c, f1l, f1r, 1)
    y1 = reduced(yr.at[1], r1_send, r1_recv)

    q_copies = []
    for turn in range(2):
        sb[turn] = ps_ref[turn, mem]
    for o in range(1, n_mem):
        one = copy(sb, ps_ref.at[:, mem], q_send.at[o - 1], q_recv.at[o - 1], at(0, 0, o))
        one.start()
        q_copies.append(one)

    def summed(x):
        return jnp.sum(jnp.sum(x, axis=0, keepdims=True), axis=1, keepdims=True)

    lane = iota((8, cols), 1)
    sums = jnp.zeros((8, cols), F32)
    for number, value in enumerate((t0 * y0, t1 * y0, t1 * y1, y1 * (obs[mem] * y1))):
        sums = jnp.where(lane == number, summed(value), sums)

    tail = []

    def total_over(value, slots, me, count, send, recv, step):
        slots[me] = value
        copies = []
        for o in range(1, count):
            one = copy(slots.at[me], slots.at[me], send.at[o - 1], recv.at[o - 1], at(*(o * s for s in step)))
            one.start()
            copies.append(one)
        for one in copies:
            one.wait_recv()
        tail.extend(copies)
        out = slots[0]
        for other in range(1, count):
            out = out + slots[other]
        return out

    sums = total_over(sums, gather_mem, mem, n_mem, sm_send, sm_recv, (0, 0, 1))
    sums = total_over(sums, gather_lat, lat, n_lat, sa_send, sa_recv, (0, 1, 0))
    sums = total_over(sums, gather_lon, lon, n_lon, so_send, so_recv, (1, 0, 0))
    row = sums[0:1]

    def pick(number):
        return jnp.sum(jnp.where(iota((1, cols), 1) == number, row, 0.0), axis=1, keepdims=True)

    rr = pick(0)
    u, v, s = pick(1) / rr, pick(2) / rr, pick(3) / rr
    alpha = 1.0 / (1.0 + u)
    beta = (v - u * u) * alpha * alpha
    g, h = 1.0 - alpha + beta, -alpha
    alpha_next = beta / (g * g * (1.0 + u) + 2.0 * g * h * (u + v) + h * h * (v + s))
    lam_ref[...] = jnp.where(lane == 0, alpha + alpha_next * g, alpha_next * h)

    for one in q_copies:
        one.wait()
    for one in a_copies + f0_copies + g_copies + f1_copies + tail:
        one.wait_send()


def per_device(n_lon, n_lat, n_mem, anomalies, spread, obs_index, innovation, obs_weight, band_width):
    members, levels, rows, cols = anomalies.shape
    ext = rows + 2 * PAD
    count = obs_index.shape[-1]
    vmem, dma = pltpu.VMEM, pltpu.SemaphoreType.DMA
    dims = (n_lon, n_lat, n_mem, members, levels, rows, cols)
    whole = pl.BlockSpec(memory_space=pltpu.VMEM)
    parts, static, lam = pl.pallas_call(
        lambda *refs: kernel(dims, *refs),
        out_shape=(
            jax.ShapeDtypeStruct((2, members, levels, rows, cols), F32),
            jax.ShapeDtypeStruct((2, levels, rows, cols), F32),
            jax.ShapeDtypeStruct((8, cols), F32),
        ),
        in_specs=[pl.BlockSpec(memory_space=pltpu.SMEM)] + [whole] * 5,
        out_specs=(whole, whole, whole),
        scratch_shapes=[
            vmem((members, levels, ext, cols), BF16),
            vmem((members, rows, cols), BF16), vmem((members, rows, cols), BF16),
            vmem((members, ext, cols), BF16), vmem((members, ext, cols), BF16),
            vmem((levels + 1, ext, cols), F32),
            vmem((2, rows, cols), F32), vmem((2, rows, cols), F32),
            vmem((2, ext, cols), F32), vmem((2, ext, cols), F32),
            vmem((levels, ext, cols), F32),
            vmem((1, rows, cols), F32), vmem((1, rows, cols), F32),
            vmem((1, ext, cols), F32), vmem((1, ext, cols), F32),
            vmem((levels, rows, cols), F32),
            vmem((levels, 9 * cols, 2 * cols), BF16),
            vmem((2, levels, 2 * rows, ext), BF16),
            vmem((members * ext, 6 * cols), BF16),
            vmem((members * ext, 2 * cols), F32),
            vmem((2, rows, cols), F32),
            vmem((levels, rows, cols), F32),
            vmem((2, n_mem - 1, rows, cols), F32),
            vmem((rows, cols), F32),
            vmem((n_mem, 8, cols), F32), vmem((n_lat, 8, cols), F32), vmem((n_lon, 8, cols), F32),
        ]
        + [dma((8,))] * 6
        + [dma((n_mem - 1,))] * 8
        + [dma((n_mem - 1,))] * 2
        + [dma((n_lat - 1,))] * 2
        + [dma((n_lon - 1,))] * 2,
        compiler_params=pltpu.CompilerParams(
            collective_id=0, has_side_effects=True, vmem_limit_bytes=48 * 1024 * 1024
        ),
    )(
        band_width, anomalies, spread, obs_index.reshape(1, count), innovation.reshape(1, count),
        obs_weight.reshape(1, count),
    )
    near, far = lam[0, 0], lam[0, 1]
    return near * parts[0] + far * parts[1], near * static[0] + far * static[1]


def solution(mesh):
    n_lon, n_lat, n_mem = (mesh.shape[name] for name in ("lon", "lat", "mem"))
    return jax.shard_map(
        lambda *args: per_device(n_lon, n_lat, n_mem, *args),
        mesh=mesh,
        in_specs=(
            P("mem", None, "lon", "lat"),
            P(None, "lon", "lat"),
            P("lon", "lat", None),
            P("lon", "lat", None),
            P("lon", "lat", None),
            P(),
        ),
        out_specs=(P("mem", None, "lon", "lat"), P(None, "lon", "lat")),
        check_vma=False,
    )
```

```python
import math

import jax
import jax.numpy as jnp
from jax import lax
from jax.experimental import pallas as pl
from jax.experimental.pallas import tpu as pltpu
from jax.sharding import PartitionSpec as P

BAND = 12
HALO = 2 * BAND
PAD = 32
CHUNKS = 4
hybrid_ens = 0.75
hybrid_static = 0.25
F32, BF16 = jnp.float32, jnp.bfloat16
HI = lax.Precision.HIGHEST
MESH = pl.DeviceIdType.MESH
AROUND = [(dx, dy) for dy in (0, 1, -1) for dx in (1, -1, 0) if (dx, dy) != (0, 0)]


def iota(shape, axis):
    return lax.broadcasted_iota(jnp.int32, shape, axis)


def dot(a, b, precision=None):
    return jnp.dot(a, b, preferred_element_type=F32, precision=precision)


def split(x):
    high = x.astype(BF16)
    return high, (x - high.astype(F32)).astype(BF16)


def kernel(dims, band_any, a_any, s_any, idx_any, inn_any, wt_any, ens_out, static_out,
           band_ref, idx_ref, inn_ref, wt_ref, ac, kl, kr, hl, hr, f0c, k0l, k0r, f0l, f0r, f1c, k1l, k1r, f1l, f1r,
           obs, mlat, nlon, xs, ub, us, p_ref, ps_ref, sl, y_ref, yr, t1_ref, gather_plane, gather_lon,
           in_sem, a_send, a_recv, f0_send, f0_recv, f1_send, f1_recv, r0_send, r0_recv, r1_send, r1_recv,
           g_send, g_recv, q0_send, q0_recv, q1_send, q1_recv, sp_send, sp_recv, so_send, so_recv, out_sem):
    n_lon, n_lat, n_mem, members, levels, rows, cols = dims
    lon, lat, mem = lax.axis_index("lon"), lax.axis_index("lat"), lax.axis_index("mem")
    ce2 = hybrid_ens / (members * n_mem)
    cs2 = hybrid_static
    ext = rows + 2 * PAD

    def at(dlon=0, dlat=0, dmem=0):
        return {
            "lon": lax.rem(lon + (dlon + n_lon), n_lon),
            "lat": lax.rem(lat + (dlat + n_lat), n_lat),
            "mem": lax.rem(mem + (dmem + n_mem), n_mem),
        }

    def copy(src, dst, send, recv, device):
        return pltpu.make_async_remote_copy(
            src_ref=src, dst_ref=dst, send_sem=send, recv_sem=recv, device_id=device, device_id_type=MESH
        )

    plane = [(0, ol, om) for ol in range(n_lat) for om in range(n_mem) if (ol, om) != (0, 0)]
    line = [(o, 0, 0) for o in range(1, n_lon)]
    partners = sorted({(dx % n_lon, dy % n_lat, 0) for dx, dy in AROUND} | set(plane) | set(line))
    barrier = pltpu.get_barrier_semaphore()
    for partner in partners:
        pl.semaphore_signal(barrier, inc=1, device_id=at(*partner), device_id_type=MESH)

    own = pl.ds(PAD, rows)
    inputs = [
        pltpu.make_async_copy(src, dst, in_sem.at[number])
        for number, (src, dst) in enumerate((
            (a_any, ac.at[:, :, own, :]), (s_any.at[mem], f0c.at[levels, own, :]), (band_any, band_ref),
            (idx_any, idx_ref), (inn_any, inn_ref), (wt_any, wt_ref),
        ))
    ]
    for one in inputs:
        one.start()
    low, high = pl.ds(PAD - HALO, HALO), pl.ds(PAD + rows, HALO)
    first, last = pl.ds(0, HALO), pl.ds(rows - HALO, HALO)

    sel_row, sel_col = iota((levels * cols, 2 * cols), 0), iota((levels * cols, 2 * cols), 1)
    sel_level, sel_lat = sel_row // cols, lax.rem(sel_row, cols)
    spot = lax.rem(sel_col, cols) - HALO * sel_level
    wanted = jnp.where(sel_col < cols, spot + (cols - HALO), spot)
    select = jnp.where((spot >= 0) & (spot < HALO) & (sel_lat == wanted), 1.0, 0.0)

    for one in inputs:
        one.wait()
    packed = dot(
        jnp.concatenate([ac[:, l, own, :].reshape(members * rows, cols) for l in range(levels)], axis=1),
        select.astype(BF16),
    ).astype(BF16)
    kl[...] = packed[:, :cols].reshape(members, rows, cols)
    kr[...] = packed[:, cols:].reshape(members, rows, cols)
    edges = (pl.ds(0, PAD - HALO), pl.ds(PAD + rows + HALO, PAD - HALO))
    for edge in edges:
        ac[:, :, edge, :] = jnp.zeros((members, levels, PAD - HALO, cols), BF16)
        for ref in (hl, hr):
            ref[:, edge, :] = jnp.zeros((members, PAD - HALO, cols), BF16)
        for ref in (f0c, f0l, f0r, f1c, f1l, f1r):
            ref[:, edge, :] = jnp.zeros((ref.shape[0], PAD - HALO, cols), F32)

    pl.semaphore_wait(barrier, len(partners))

    from_rows = {1: last, -1: first, 0: pl.ds(0, rows)}
    field_rows = {1: pl.ds(PAD + rows - HALO, HALO), -1: pl.ds(PAD, HALO)}
    to_rows = {1: low, -1: high, 0: own}

    def halo(centre, left, right, packed_left, packed_right, send, recv, chunk=None):
        copies = []
        for number, (dx, dy) in enumerate(AROUND):
            if dy == 0:
                if chunk is None:
                    src, dst = centre.at[:, field_rows[dx], :], centre.at[:, to_rows[dx], :]
                else:
                    src, dst = centre.at[chunk, :, field_rows[dx], :], centre.at[chunk, :, to_rows[dx], :]
            else:
                every = slice(None) if chunk is None else chunk
                src = (packed_left if dy == 1 else packed_right).at[every, from_rows[dx], :]
                dst = (left if dy == 1 else right).at[every, to_rows[dx], :]
            one = copy(src, dst, send.at[number], recv.at[number], at(dx, dy))
            one.start()
            copies.append(one)
        return copies

    batch = members // CHUNKS

    def send_chunk(number):
        return halo(ac, hl, hr, kl, kr, a_send.at[number], a_recv.at[number], pl.ds(number * batch, batch))

    a_copies = [send_chunk(0)]

    index = idx_ref[...]
    weight = wt_ref[...]
    at_row, at_col = index // cols, lax.rem(index, cols)
    count = index.shape[1]
    columns = jnp.where(iota((cols, count), 0) == at_col, 1.0, 0.0).astype(BF16)

    def thirds(v):
        one = v.astype(BF16).astype(F32)
        two = (v - one).astype(BF16).astype(F32)
        return [one, two, v - one - two]

    terms = thirds(weight) + thirds(weight * inn_ref[...])

    def level_fields(l, carry):
        here = (iota((rows, count), 0) + rows * l) == at_row
        stacked = jnp.concatenate([jnp.where(here, t, 0.0).astype(BF16) for t in terms], axis=0)
        sums = lax.dot_general(stacked, columns, (((1,), (1,)), ((), ())), preferred_element_type=F32)
        obs[l] = sums[0:rows] + sums[rows:2 * rows] + sums[2 * rows:3 * rows]
        f0c[l, own, :] = sums[3 * rows:4 * rows] + sums[4 * rows:5 * rows] + sums[5 * rows:]
        return carry

    lax.fori_loop(0, levels, level_fields, 0)

    def pack(centre, left, right, extra=0.0):
        both = dot(jnp.concatenate([centre[l, own, :] for l in range(levels)], axis=1), select, HI) + extra
        left[0] = both[:, :cols]
        right[0] = both[:, cols:]

    spare = levels * HALO
    spot = lax.rem(iota((cols, 2 * cols), 1), cols) - spare
    wanted = jnp.where(iota((cols, 2 * cols), 1) < cols, spot + (cols - HALO), spot)
    place = jnp.where((spot >= 0) & (spot < HALO) & (iota((cols, 2 * cols), 0) == wanted), 1.0, 0.0)
    pack(f0c, k0l, k0r, dot(f0c[levels, own, :], place, HI))
    f0_copies = halo(f0c, f0l, f0r, k0l, k0r, f0_send, f0_recv)
    a_copies.append(send_chunk(1))
    r, c = iota((cols, cols), 0), iota((cols, cols), 1)
    inside_low = jnp.where(lat > 0, 1.0, 0.0).astype(F32)
    inside_high = jnp.where(lat < n_lat - 1, 1.0, 0.0).astype(F32)
    offsets = iota((8, cols), 1) - BAND

    def level_matrices(l, carry):
        def band_of(which):
            width = jnp.full((1, 1), band_ref[which, l].astype(F32), F32)

            def raw(diff):
                d = diff.astype(F32)
                ratio = d / (0.5 * width)
                return jnp.where(jnp.abs(d) <= width, jnp.exp(-0.5 * (ratio * ratio)), 0.0)

            total = jnp.sum(raw(offsets), axis=1, keepdims=True)[0:1]
            return lambda diff: raw(diff) / total

        band = band_of(1)
        spot = r - HALO * l
        valid = jnp.where((spot >= 0) & (spot < HALO), 1.0, 0.0)
        d0, dm, dp = band(r - c), band(r - cols - c), band(r + cols - c)
        from_low = spot + (cols - HALO)
        dml, d0l = band(from_low - cols - c) * valid, band(from_low - c) * valid
        dpr, d0r = band(spot + cols - c) * valid, band(spot - c) * valid
        twice = [
            dot(d0, d0, HI) + inside_low * dot(dp, dm, HI) + inside_high * dot(dm, dp, HI),
            inside_low * (dot(d0l, dm, HI) + dot(dml, d0, HI)),
            inside_high * (dot(d0r, dp, HI) + dot(dpr, d0, HI)),
        ]
        once = [d0, inside_low * dml, inside_high * dpr]
        for part in range(3):
            hi, lo = split(jnp.concatenate([twice[part], once[part]], axis=1))
            mlat[l, part * cols:(part + 1) * cols, :] = hi
            mlat[l, (3 + part) * cols:(4 + part) * cols, :] = hi
            mlat[l, (6 + part) * cols:(7 + part) * cols, :] = lo
        band = band_of(0)
        near = band(iota((rows, ext), 0) + PAD - iota((rows, ext), 1))
        far = band(iota((ext, ext), 0) - iota((ext, ext), 1))
        for which, matrix in enumerate((dot(near, far, HI), near)):
            hi, lo = split(matrix)
            nlon[which, l, 0:rows, :] = hi
            nlon[which, l, rows:2 * rows, :] = lo
        return carry

    lax.fori_loop(0, levels, level_matrices, 0)

    for one in f0_copies:
        one.wait_recv()
    a_copies.append(send_chunk(2))
    realign = jnp.where((r - spare == c - HALO * mem) & (r >= spare) & (r < spare + HALO), 1.0, 0.0)
    sl[0] = dot(f0l[0], realign, HI)
    sl[1] = dot(f0r[0], realign, HI)

    def lon_pass(l, u_hi, u_lo, which):
        tall = dot(nlon[which, l], u_hi)
        return tall[0:rows] + tall[rows:] + dot(nlon[which, l, 0:rows, :], u_lo)

    def apply_members(centre, left, right, start, count):
        zl, zr = left[0], right[0]
        z = [centre[l] for l in range(levels)]
        chunk = pl.ds(start * ext, count * ext)
        for k in range(start, start + count):
            spans = pl.ds(k * ext, ext)
            for part, (rim, zz) in enumerate(((hl, zl), (hr, zr))):
                hi, lo = split(rim[k].astype(F32) * zz)
                for l in range(levels):
                    xs[l, spans, (1 + part) * cols:(2 + part) * cols] = hi
                    xs[l, spans, (4 + part) * cols:(5 + part) * cols] = lo
            for l in range(levels):
                hi, lo = split(ac[k, l].astype(F32) * z[l])
                xs[l, spans, 0:cols] = hi
                xs[l, spans, 3 * cols:4 * cols] = lo
        for l in range(levels):
            ub[l, chunk, :] = dot(xs[l, chunk, :], mlat[l, 0:6 * cols, :]) + dot(
                xs[l, chunk, 0:3 * cols], mlat[l, 6 * cols:, :]
            )
        for l in range(levels):
            total = jnp.zeros((rows, cols), F32)
            for k in range(start, start + count):
                hi, lo = split(ub[l, pl.ds(k * ext, ext), 0:cols])
                total += ac[k, l, own, :].astype(F32) * lon_pass(l, hi, lo, 0)
            y_ref[l] = ce2 * total if start == 0 else y_ref[l] + ce2 * total

    def apply_static(centre, left, right):
        his, los = [], []
        for stat, z in ((f0c[levels], centre[mem]), (sl[0], left[0]), (sl[1], right[0])):
            hi, lo = split(stat * z)
            his.append(hi)
            los.append(lo)
        u = dot(jnp.concatenate(his + los, axis=1), mlat[mem, 0:6 * cols, :])
        us[...] = u + dot(jnp.concatenate(his, axis=1), mlat[mem, 6 * cols:, :])
        hi, lo = split(us[:, 0:cols])
        y_ref[mem] = y_ref[mem] + cs2 * f0c[levels, own, :] * lon_pass(mem, hi, lo, 0)

    def parts(turn, which):
        for l in which:
            for k in range(members):
                hi, lo = split(ub[l, pl.ds(k * ext, ext), cols:2 * cols])
                p_ref[turn, k, l] = math.sqrt(ce2) * lon_pass(l, hi, lo, 1)

    def static_part(turn, send, recv):
        hi, lo = split(us[:, cols:2 * cols])
        ps_ref[turn, mem] = math.sqrt(cs2) * lon_pass(mem, hi, lo, 1)
        copies = []
        for o in range(1, n_mem):
            one = copy(
                ps_ref.at[turn, mem], ps_ref.at[turn, mem], send.at[o - 1], recv.at[o - 1], at(0, 0, o)
            )
            one.start()
            copies.append(one)
        return copies

    def scatter_sum(slots, send, recv):
        copies = []
        for o in range(1, n_mem):
            peer = lax.rem(mem + o, n_mem)
            one = copy(y_ref.at[peer], slots.at[o - 1], send.at[o - 1], recv.at[o - 1], at(0, 0, o))
            one.start()
            copies.append(one)
        return copies

    def finish_sum(copies, slots):
        for one in copies:
            one.wait()
        total = y_ref[mem]
        for o in range(n_mem - 1):
            total = total + slots[o]
        return total

    for number in range(CHUNKS):
        for one in a_copies[number]:
            one.wait_recv()
        apply_members(f0c, f0l, f0r, number * batch, batch)
        if number + 3 < CHUNKS:
            a_copies.append(send_chunk(number + 3))
    apply_static(f0c, f0l, f0r)
    r0_copies = scatter_sum(yr.at[0], r0_send, r0_recv)
    parts(0, (0, 1))
    y0 = finish_sum(r0_copies, yr.at[0])
    t0 = f0c[mem, own, :]
    t1 = obs[mem] * y0
    t1_ref[...] = t1
    f1c[mem, own, :] = t1
    g_copies = []
    for o in range(1, n_mem):
        one = copy(t1_ref, f1c.at[mem, own, :], g_send.at[o - 1], g_recv.at[o - 1], at(0, 0, o))
        one.start()
        g_copies.append(one)
    parts(0, (2, 3))
    for one in g_copies:
        one.wait_recv()
    pack(f1c, k1l, k1r)
    f1_copies = halo(f1c, f1l, f1r, k1l, k1r, f1_send, f1_recv)
    q0_copies = static_part(0, q0_send, q0_recv)
    for one in f1_copies:
        one.wait_recv()
    apply_members(f1c, f1l, f1r, 0, members)
    apply_static(f1c, f1l, f1r)
    r1_copies = scatter_sum(yr.at[1], r1_send, r1_recv)
    parts(1, range(levels))
    y1 = finish_sum(r1_copies, yr.at[1])

    def summed(x):
        return jnp.sum(jnp.sum(x, axis=0, keepdims=True), axis=1, keepdims=True)

    lane = iota((8, cols), 1)
    sums = jnp.zeros((8, cols), F32)
    for number, value in enumerate((t0 * y0, t1 * y0, t1 * y1, y1 * (obs[mem] * y1))):
        sums = jnp.where(lane == number, summed(value), sums)

    def total_start(value, slots, me, offsets, send, recv):
        slots[me] = value
        copies = []
        for number, offset in enumerate(offsets):
            one = copy(slots.at[me], slots.at[me], send.at[number], recv.at[number], at(*offset))
            one.start()
            copies.append(one)
        return copies

    def total_finish(slots, copies):
        for one in copies:
            one.wait_recv()
        out = slots[0]
        for other in range(1, len(copies) + 1):
            out = out + slots[other]
        return out

    plane_copies = total_start(sums, gather_plane, lat * n_mem + mem, plane, sp_send, sp_recv)
    sums = total_finish(gather_plane, plane_copies)
    line_copies = total_start(sums, gather_lon, lon, line, so_send, so_recv)
    q1_copies = static_part(1, q1_send, q1_recv)
    sums = total_finish(gather_lon, line_copies)
    row = sums[0:1]

    def pick(number):
        return jnp.sum(jnp.where(iota((1, cols), 1) == number, row, 0.0), axis=1, keepdims=True)

    rr = pick(0)
    u, v, s = pick(1) / rr, pick(2) / rr, pick(3) / rr
    alpha = 1.0 / (1.0 + u)
    beta = (v - u * u) * alpha * alpha
    g, h = 1.0 - alpha + beta, -alpha
    alpha_next = beta / (g * g * (1.0 + u) + 2.0 * g * h * (u + v) + h * h * (v + s))
    near, far = alpha + alpha_next * g, alpha_next * h
    outs = []
    for k in range(members):
        p_ref[0, k] = near * p_ref[0, k] + far * p_ref[1, k]
        outs.append(pltpu.make_async_copy(p_ref.at[0, k], ens_out.at[k], out_sem.at[k]))
        outs[-1].start()
    for one in q0_copies + q1_copies:
        one.wait()
    y_ref[...] = near * ps_ref[0] + far * ps_ref[1]
    outs.append(pltpu.make_async_copy(y_ref, static_out, out_sem.at[members]))
    outs[-1].start()
    for one in outs:
        one.wait()
    for copies in a_copies:
        for one in copies:
            one.wait_send()
    for one in f0_copies + g_copies + f1_copies + plane_copies + line_copies:
        one.wait_send()


def per_device(n_lon, n_lat, n_mem, anomalies, spread, obs_index, innovation, obs_weight, band_width):
    members, levels, rows, cols = anomalies.shape
    ext = rows + 2 * PAD
    count = obs_index.shape[-1]
    vmem, dma = pltpu.VMEM, pltpu.SemaphoreType.DMA
    dims = (n_lon, n_lat, n_mem, members, levels, rows, cols)
    far = pl.BlockSpec(memory_space=pltpu.HBM)
    return pl.pallas_call(
        lambda *refs: kernel(dims, *refs),
        out_shape=(
            jax.ShapeDtypeStruct((members, levels, rows, cols), F32),
            jax.ShapeDtypeStruct((levels, rows, cols), F32),
        ),
        in_specs=[far] * 6,
        out_specs=(far, far),
        scratch_shapes=[
            pltpu.SMEM((2, levels), jnp.int32),
            vmem((1, count), jnp.int32), vmem((1, count), F32), vmem((1, count), F32),
            vmem((members, levels, ext, cols), BF16),
            vmem((members, rows, cols), BF16), vmem((members, rows, cols), BF16),
            vmem((members, ext, cols), BF16), vmem((members, ext, cols), BF16),
            vmem((levels + 1, ext, cols), F32),
            vmem((1, rows, cols), F32), vmem((1, rows, cols), F32),
            vmem((1, ext, cols), F32), vmem((1, ext, cols), F32),
            vmem((levels, ext, cols), F32),
            vmem((1, rows, cols), F32), vmem((1, rows, cols), F32),
            vmem((1, ext, cols), F32), vmem((1, ext, cols), F32),
            vmem((levels, rows, cols), F32),
            vmem((levels, 9 * cols, 2 * cols), BF16),
            vmem((2, levels, 2 * rows, ext), BF16),
            vmem((levels, members * ext, 6 * cols), BF16),
            vmem((levels, members * ext, 2 * cols), F32),
            vmem((ext, 2 * cols), F32),
            vmem((2, members, levels, rows, cols), F32),
            vmem((2, levels, rows, cols), F32),
            vmem((2, ext, cols), F32),
            vmem((levels, rows, cols), F32),
            vmem((2, n_mem - 1, rows, cols), F32),
            vmem((rows, cols), F32),
            vmem((n_lat * n_mem, 8, cols), F32), vmem((n_lon, 8, cols), F32),
        ]
        + [dma((6,))]
        + [dma((CHUNKS, 8))] * 2
        + [dma((8,))] * 4
        + [dma((n_mem - 1,))] * 10
        + [dma((n_lat * n_mem - 1,))] * 2
        + [dma((n_lon - 1,))] * 2
        + [dma((members + 1,))],
        compiler_params=pltpu.CompilerParams(
            collective_id=0, has_side_effects=True, vmem_limit_bytes=63 * 1024 * 1024
        ),
    )(
        band_width, anomalies, spread, obs_index.reshape(1, count), innovation.reshape(1, count),
        obs_weight.reshape(1, count),
    )


def solution(mesh):
    n_lon, n_lat, n_mem = (mesh.shape[name] for name in ("lon", "lat", "mem"))
    return jax.shard_map(
        lambda *args: per_device(n_lon, n_lat, n_mem, *args),
        mesh=mesh,
        in_specs=(
            P("mem", None, "lon", "lat"),
            P(None, "lon", "lat"),
            P("lon", "lat", None),
            P("lon", "lat", None),
            P("lon", "lat", None),
            P(),
        ),
        out_specs=(P("mem", None, "lon", "lat"), P(None, "lon", "lat")),
        check_vma=False,
    )
```

```python
import math

import jax
import jax.numpy as jnp
from jax import lax
from jax.experimental import pallas as pl
from jax.experimental.pallas import tpu as pltpu
from jax.sharding import PartitionSpec as P

BAND = 12
HALO = 2 * BAND
PAD = HALO
CHUNKS = 4
hybrid_ens = 0.75
hybrid_static = 0.25
F32, BF16 = jnp.float32, jnp.bfloat16
HI = lax.Precision.HIGHEST
MESH = pl.DeviceIdType.MESH
AROUND = [(dx, dy) for dy in (0, 1, -1) for dx in (1, -1, 0) if (dx, dy) != (0, 0)]


def iota(shape, axis):
    return lax.broadcasted_iota(jnp.int32, shape, axis)


def dot(a, b, precision=None):
    return jnp.dot(a, b, preferred_element_type=F32, precision=precision)


def split(x):
    high = x.astype(BF16)
    return high, (x - high.astype(F32)).astype(BF16)


def kernel(dims, band_any, a_any, s_any, idx_any, inn_any, wt_any, ens_out, static_out, lam_out,
           band_ref, idx_ref, inn_ref, wt_ref, ac, kl, kr, hl, hr, f0c, k0l, k0r, f0l, f0r, f1c, k1l, k1r, f1l, f1r,
           obs, mlat, nlon, xs, ub, us, p_ref, ps_ref, lam_ref, sl, y_ref, yr, t1_ref, gather_plane, gather_lon,
           in_sem, a_send, a_recv, f0_send, f0_recv, f1_send, f1_recv, r0_send, r0_recv, r1_send, r1_recv,
           g_send, g_recv, c1_send, c1_recv, q0_send, q0_recv, q1_send, q1_recv, sp_send, sp_recv, so_send, so_recv, out_sem):
    n_lon, n_lat, n_mem, members, levels, rows, cols = dims
    lon, lat, mem = lax.axis_index("lon"), lax.axis_index("lat"), lax.axis_index("mem")
    ce2 = hybrid_ens / (members * n_mem)
    cs2 = hybrid_static
    ext = rows + 2 * PAD

    def at(dlon=0, dlat=0, dmem=0):
        return {
            "lon": lax.rem(lon + (dlon + n_lon), n_lon),
            "lat": lax.rem(lat + (dlat + n_lat), n_lat),
            "mem": lax.rem(mem + (dmem + n_mem), n_mem),
        }

    def copy(src, dst, send, recv, device):
        return pltpu.make_async_remote_copy(
            src_ref=src, dst_ref=dst, send_sem=send, recv_sem=recv, device_id=device, device_id_type=MESH
        )
    parity = lax.rem(lon, 2)
    across = 1 - 2 * parity
    plane = [(tx * across, ol, om) for tx in range(2) for ol in range(n_lat) for om in range(n_mem)][1:]
    line = [(o, 0, 0) for o in range(2, n_lon, 2)]
    partners = plane + line + [(-across, dy, 0) for dy in (0, 1, -1)] + [(-across, 0, o) for o in range(1, n_mem)]
    barrier = pltpu.get_barrier_semaphore()
    for partner in partners:
        pl.semaphore_signal(barrier, inc=1, device_id=at(*partner), device_id_type=MESH)

    own = pl.ds(PAD, rows)
    inputs = [
        pltpu.make_async_copy(src, dst, in_sem.at[number])
        for number, (src, dst) in enumerate((
            (a_any, ac.at[:, :, own, :]), (s_any.at[mem], f0c.at[levels, own, :]), (band_any, band_ref),
            (idx_any, idx_ref), (inn_any, inn_ref), (wt_any, wt_ref),
        ))
    ]
    for one in inputs:
        one.start()
    low, high = pl.ds(PAD - HALO, HALO), pl.ds(PAD + rows, HALO)
    first, last = pl.ds(0, HALO), pl.ds(rows - HALO, HALO)
    sel_row, sel_col = iota((levels * cols, 2 * cols), 0), iota((levels * cols, 2 * cols), 1)
    sel_level, sel_lat = sel_row // cols, lax.rem(sel_row, cols)
    spot = lax.rem(sel_col, cols) - HALO * sel_level
    wanted = jnp.where(sel_col < cols, spot + (cols - HALO), spot)
    select = jnp.where((spot >= 0) & (spot < HALO) & (sel_lat == wanted), 1.0, 0.0)

    for one in inputs:
        one.wait()
    packed = dot(
        jnp.concatenate([ac[:, l, own, :].reshape(members * rows, cols) for l in range(levels)], axis=1),
        select.astype(BF16),
    ).astype(BF16)
    kl[...] = packed[:, :cols].reshape(members, rows, cols)
    kr[...] = packed[:, cols:].reshape(members, rows, cols)
    pl.semaphore_wait(barrier, len(partners))

    from_rows = {1: last, -1: first, 0: pl.ds(0, rows)}
    field_rows = {1: pl.ds(PAD + rows - HALO, HALO), -1: pl.ds(PAD, HALO)}
    to_rows = {1: low, -1: high, 0: own}

    def halo(centre, left, right, packed_left, packed_right, send, recv, chunk=None, skip=0):
        copies = []
        for number, (dx, dy) in enumerate(AROUND[skip:]):
            if dy == 0:
                if chunk is None:
                    src, dst = centre.at[:, field_rows[dx], :], centre.at[:, to_rows[dx], :]
                else:
                    src, dst = centre.at[chunk, :, field_rows[dx], :], centre.at[chunk, :, to_rows[dx], :]
            else:
                every = slice(None) if chunk is None else chunk
                src = (packed_left if dy == 1 else packed_right).at[every, from_rows[dx], :]
                dst = (left if dy == 1 else right).at[every, to_rows[dx], :]
            one = copy(src, dst, send.at[number], recv.at[number], at(dx, dy))
            one.start()
            copies.append(one)
        return copies

    batch = members // CHUNKS

    def send_chunk(number):
        return halo(ac, hl, hr, kl, kr, a_send.at[number], a_recv.at[number], pl.ds(number * batch, batch))
    a_copies = [send_chunk(0)]
    index = idx_ref[...]
    weight = wt_ref[...]
    at_row, at_col = index // cols, lax.rem(index, cols)
    count = index.shape[1]
    columns = jnp.where(iota((cols, count), 0) == at_col, 1.0, 0.0).astype(BF16)

    def thirds(v):
        one = v.astype(BF16).astype(F32)
        two = (v - one).astype(BF16).astype(F32)
        return [one, two, v - one - two]

    terms = thirds(weight) + thirds(weight * inn_ref[...])

    def level_fields(l, carry):
        here = (iota((rows, count), 0) + rows * l) == at_row
        stacked = jnp.concatenate([jnp.where(here, t, 0.0).astype(BF16) for t in terms], axis=0)
        sums = lax.dot_general(stacked, columns, (((1,), (1,)), ((), ())), preferred_element_type=F32)
        obs[l] = sums[0:rows] + sums[rows:2 * rows] + sums[2 * rows:3 * rows]
        f0c[l, own, :] = sums[3 * rows:4 * rows] + sums[4 * rows:5 * rows] + sums[5 * rows:]
        return carry

    lax.fori_loop(0, levels, level_fields, 0)

    select16 = select.astype(BF16)

    def select_exact(x, chosen):
        terms = dot(jnp.concatenate([t.astype(BF16) for t in thirds(x)], axis=0), chosen)
        return terms[0:rows] + terms[rows:2 * rows] + terms[2 * rows:]

    def pack(centre, left, right, extra=0.0):
        whole = jnp.concatenate([centre[l, own, :] for l in range(levels)], axis=1)
        both = select_exact(whole, select16) + extra
        left[0] = both[:, :cols]
        right[0] = both[:, cols:]

    spare = levels * HALO
    spot = lax.rem(iota((cols, 2 * cols), 1), cols) - spare
    wanted = jnp.where(iota((cols, 2 * cols), 1) < cols, spot + (cols - HALO), spot)
    place = jnp.where((spot >= 0) & (spot < HALO) & (iota((cols, 2 * cols), 0) == wanted), 1.0, 0.0)
    pack(f0c, k0l, k0r, select_exact(f0c[levels, own, :], place.astype(BF16)))
    f0_copies = halo(f0c, f0l, f0r, k0l, k0r, f0_send, f0_recv)
    a_copies.append(send_chunk(1))
    r, c = iota((cols, cols), 0), iota((cols, cols), 1)
    inside_low = jnp.where(lat > 0, 1.0, 0.0).astype(F32)
    inside_high = jnp.where(lat < n_lat - 1, 1.0, 0.0).astype(F32)
    offsets = iota((8, cols), 1) - BAND

    def level_matrices(l, carry):
        def band_of(which):
            width = jnp.full((1, 1), band_ref[which, l].astype(F32), F32)

            def raw(diff):
                d = diff.astype(F32)
                ratio = d / (0.5 * width)
                return jnp.where(jnp.abs(d) <= width, jnp.exp(-0.5 * (ratio * ratio)), 0.0)

            total = jnp.sum(raw(offsets), axis=1, keepdims=True)[0:1]
            return lambda diff: raw(diff) / total

        band = band_of(1)
        spot = r - HALO * l
        valid = jnp.where((spot >= 0) & (spot < HALO), 1.0, 0.0)
        d0, dm, dp = band(r - c), band(r - cols - c), band(r + cols - c)
        from_low = spot + (cols - HALO)
        dml, d0l = band(from_low - cols - c) * valid, band(from_low - c) * valid
        dpr, d0r = band(spot + cols - c) * valid, band(spot - c) * valid
        twice = [
            dot(d0, d0, HI) + inside_low * dot(dp, dm, HI) + inside_high * dot(dm, dp, HI),
            inside_low * (dot(d0l, dm, HI) + dot(dml, d0, HI)),
            inside_high * (dot(d0r, dp, HI) + dot(dpr, d0, HI)),
        ]
        once = [d0, inside_low * dml, inside_high * dpr]
        for part in range(3):
            hi, lo = split(jnp.concatenate([twice[part], once[part]], axis=1))
            mlat[l, part * cols:(part + 1) * cols, :] = hi
            mlat[l, (3 + part) * cols:(4 + part) * cols, :] = hi
            mlat[l, (6 + part) * cols:(7 + part) * cols, :] = lo
        band = band_of(0)
        near = band(iota((rows, ext), 0) + PAD - iota((rows, ext), 1))
        far = band(iota((ext, ext), 0) - iota((ext, ext), 1))
        for which, matrix in enumerate((dot(near, far, HI), near)):
            hi, lo = split(matrix)
            nlon[which, l, 0:rows, :] = hi
            nlon[which, l, rows:2 * rows, :] = lo
        return carry

    lax.fori_loop(0, levels, level_matrices, 0)
    a_copies.append(send_chunk(2))
    for one in f0_copies:
        one.wait_recv()
    a_copies.append(send_chunk(3))
    realign = jnp.where((r - spare == c - HALO * mem) & (r >= spare) & (r < spare + HALO), 1.0, 0.0)
    sl[0] = dot(f0l[0], realign, HI)
    sl[1] = dot(f0r[0], realign, HI)

    def lon_pass(l, u_hi, u_lo, which):
        tall = dot(nlon[which, l], u_hi)
        return tall[0:rows] + tall[rows:] + dot(nlon[which, l, 0:rows, :], u_lo)

    def apply_members(centre, left, right, start, count):
        zl, zr = left[0], right[0]
        z = [centre[l] for l in range(levels)]
        chunk = pl.ds(start * ext, count * ext)
        for k in range(start, start + count):
            spans = pl.ds(k * ext, ext)
            for part, (rim, zz) in enumerate(((hl, zl), (hr, zr))):
                hi, lo = split(rim[k].astype(F32) * zz)
                for l in range(levels):
                    xs[l, spans, (1 + part) * cols:(2 + part) * cols] = hi
                    xs[l, spans, (4 + part) * cols:(5 + part) * cols] = lo
            for l in range(levels):
                hi, lo = split(ac[k, l].astype(F32) * z[l])
                xs[l, spans, 0:cols] = hi
                xs[l, spans, 3 * cols:4 * cols] = lo
        def lat_level(l):
            ub[l, chunk, :] = dot(xs[l, chunk, :], mlat[l, 0:6 * cols, :]) + dot(
                xs[l, chunk, 0:3 * cols], mlat[l, 6 * cols:, :]
            )

        def lon_level(l):
            total = jnp.zeros((rows, cols), F32)
            for k in range(start, start + count):
                hi, lo = split(ub[l, pl.ds(k * ext, ext), 0:cols])
                total += ac[k, l, own, :].astype(F32) * lon_pass(l, hi, lo, 0)
            y_ref[l] = ce2 * total if start == 0 else y_ref[l] + ce2 * total

        for l in range(levels):
            lat_level(l)
        for l in range(levels):
            lon_level(l)

    def apply_static(centre, left, right):
        his, los = [], []
        for stat, z in ((f0c[levels], centre[mem]), (sl[0], left[0]), (sl[1], right[0])):
            hi, lo = split(stat * z)
            his.append(hi)
            los.append(lo)
        u = dot(jnp.concatenate(his + los, axis=1), mlat[mem, 0:6 * cols, :])
        us[...] = u + dot(jnp.concatenate(his, axis=1), mlat[mem, 6 * cols:, :])
        hi, lo = split(us[:, 0:cols])
        y_ref[mem] = y_ref[mem] + cs2 * f0c[levels, own, :] * lon_pass(mem, hi, lo, 0)

    def parts(turn, which):
        for l in which:
            for k in range(members):
                hi, lo = split(ub[l, pl.ds(k * ext, ext), cols:2 * cols])
                p_ref[turn, k, l] = math.sqrt(ce2) * lon_pass(l, hi, lo, 1)

    def static_part(turn, send, recv):
        hi, lo = split(us[:, cols:2 * cols])
        ps_ref[turn, mem] = math.sqrt(cs2) * lon_pass(mem, hi, lo, 1)
        copies = []
        for o in range(1, n_mem):
            one = copy(
                ps_ref.at[turn, mem], ps_ref.at[turn, mem], send.at[o - 1], recv.at[o - 1], at(0, 0, o)
            )
            one.start()
            copies.append(one)
        return copies

    def scatter_sum(slots, send, recv):
        copies = []
        for o in range(1, n_mem):
            other = lax.rem(mem + o, n_mem)
            one = copy(y_ref.at[other], slots.at[o - 1], send.at[o - 1], recv.at[o - 1], at(0, 0, o))
            one.start()
            copies.append(one)
        return copies

    def finish_sum(copies, slots):
        total = y_ref[mem]
        for o, one in enumerate(copies):
            one.wait()
            total = total + slots[o]
        return total

    for number in range(CHUNKS):
        for one in a_copies[number]:
            one.wait_recv()
        apply_members(f0c, f0l, f0r, number * batch, batch)
    r0_copies = scatter_sum(yr.at[0], r0_send, r0_recv)
    apply_static(f0c, f0l, f0r)
    parts(0, (0, 1))
    y0 = finish_sum(r0_copies, yr.at[0])
    t0 = f0c[mem, own, :]
    t1 = obs[mem] * y0
    t1_ref[...] = t1
    f1c[mem, own, :] = t1
    g_copies, c1_copies = [], []
    for o in range(1, n_mem):
        one = copy(t1_ref, f1c.at[mem, own, :], g_send.at[o - 1], g_recv.at[o - 1], at(0, 0, o))
        one.start()
        g_copies.append(one)
    for number, dx in enumerate((1, -1)):
        for o in range(n_mem):
            one = copy(
                t1_ref.at[from_rows[dx], :], f1c.at[mem, to_rows[dx], :],
                c1_send.at[number, o], c1_recv.at[number, o], at(dx, 0, o),
            )
            one.start()
            c1_copies.append(one)
    parts(0, (2, 3))
    outs = [pltpu.make_async_copy(p_ref.at[0], ens_out.at[0], out_sem.at[0])]
    outs[-1].start()
    for one in g_copies:
        one.wait_recv()
    pack(f1c, k1l, k1r)
    f1_copies = halo(f1c, f1l, f1r, k1l, k1r, f1_send, f1_recv, skip=2)
    q0_copies = static_part(0, q0_send, q0_recv)
    for one in f1_copies + c1_copies:
        one.wait_recv()
    apply_members(f1c, f1l, f1r, 0, members)
    r1_copies = scatter_sum(yr.at[1], r1_send, r1_recv)
    apply_static(f1c, f1l, f1r)
    parts(1, range(levels))
    outs.append(pltpu.make_async_copy(p_ref.at[1], ens_out.at[1], out_sem.at[1]))
    outs[-1].start()
    y1 = finish_sum(r1_copies, yr.at[1])

    def summed(x):
        return jnp.sum(jnp.sum(x, axis=0, keepdims=True), axis=1, keepdims=True)

    lane = iota((8, cols), 1)
    sums = jnp.zeros((8, cols), F32)
    for number, value in enumerate((t0 * y0, t1 * y0, t1 * y1, y1 * (obs[mem] * y1))):
        sums = jnp.where(lane == number, summed(value), sums)

    def total_start(value, slots, me, offsets, send, recv):
        slots[me] = value
        copies = []
        for number, offset in enumerate(offsets):
            one = copy(slots.at[me, 0:1, :], slots.at[me, 0:1, :], send.at[number], recv.at[number], at(*offset))
            one.start()
            copies.append(one)
        return copies

    def total_finish(slots, copies):
        for one in copies:
            one.wait_recv()
        out = slots[0, 0:1, :]
        for other in range(1, len(copies) + 1):
            out = out + slots[other, 0:1, :]
        return jnp.broadcast_to(out, (8, cols))

    plane_copies = total_start(sums, gather_plane, (parity * n_lat + lat) * n_mem + mem, plane, sp_send, sp_recv)
    sums = total_finish(gather_plane, plane_copies)
    line_copies = total_start(sums, gather_lon, lon // 2, line, so_send, so_recv)
    q1_copies = static_part(1, q1_send, q1_recv)
    sums = total_finish(gather_lon, line_copies)
    row = sums[0:1]

    def pick(number):
        return jnp.sum(jnp.where(iota((1, cols), 1) == number, row, 0.0), axis=1, keepdims=True)

    rr = pick(0)
    u, v, s = pick(1) / rr, pick(2) / rr, pick(3) / rr
    alpha = 1.0 / (1.0 + u)
    beta = (v - u * u) * alpha * alpha
    g, h = 1.0 - alpha + beta, -alpha
    alpha_next = beta / (g * g * (1.0 + u) + 2.0 * g * h * (u + v) + h * h * (v + s))
    lam_ref[...] = jnp.where(lane == 0, alpha + alpha_next * g, alpha_next * h)
    outs.append(pltpu.make_async_copy(lam_ref, lam_out, out_sem.at[2]))
    outs[-1].start()
    for one in q0_copies + q1_copies:
        one.wait()
    outs.append(pltpu.make_async_copy(ps_ref, static_out, out_sem.at[3]))
    outs[-1].start()
    for one in outs:
        one.wait()
    for copies in a_copies:
        for one in copies:
            one.wait_send()
    for one in f0_copies + g_copies + c1_copies + f1_copies + plane_copies + line_copies:
        one.wait_send()


def combine(ens_in, static_in, lam_in, ens_out, static_out, ens, static, lam, ens_sem, in_sem, out_sem):
    members = ens_out.shape[0]
    lam_copy = pltpu.make_async_copy(lam_in, lam, in_sem.at[0])
    static_copy = pltpu.make_async_copy(static_in, static, in_sem.at[1])
    lam_copy.start()
    loads = [pltpu.make_async_copy(ens_in.at[:, k], ens.at[:, k], ens_sem.at[k]) for k in range(members)]
    for one in loads:
        one.start()
    static_copy.start()
    lam_copy.wait()
    near, far = lam[0:1, 0:1], lam[0:1, 1:2]
    stores = []
    for k in range(members):
        loads[k].wait()
        ens[0, k] = near * ens[0, k] + far * ens[1, k]
        stores.append(pltpu.make_async_copy(ens.at[0, k], ens_out.at[k], out_sem.at[k]))
        stores[-1].start()
    static_copy.wait()
    static[0] = near * static[0] + far * static[1]
    stores.append(pltpu.make_async_copy(static.at[0], static_out, out_sem.at[members]))
    stores[-1].start()
    for one in stores:
        one.wait()


def per_device(n_lon, n_lat, n_mem, anomalies, spread, obs_index, innovation, obs_weight, band_width):
    members, levels, rows, cols = anomalies.shape
    ext = rows + 2 * PAD
    count = obs_index.shape[-1]
    vmem, dma = pltpu.VMEM, pltpu.SemaphoreType.DMA
    dims = (n_lon, n_lat, n_mem, members, levels, rows, cols)
    far = pl.BlockSpec(memory_space=pltpu.HBM)
    done = pl.pallas_call(
        lambda *refs: kernel(dims, *refs),
        out_shape=(
            jax.ShapeDtypeStruct((2, members, levels, rows, cols), F32),
            jax.ShapeDtypeStruct((2, levels, rows, cols), F32),
            jax.ShapeDtypeStruct((8, cols), F32),
        ),
        in_specs=[far] * 6,
        out_specs=(far, far, far),
        scratch_shapes=[
            pltpu.SMEM((2, levels), jnp.int32),
            vmem((1, count), jnp.int32), vmem((1, count), F32), vmem((1, count), F32),
            vmem((members, levels, ext, cols), BF16),
            vmem((members, rows, cols), BF16), vmem((members, rows, cols), BF16),
            vmem((members, ext, cols), BF16), vmem((members, ext, cols), BF16),
            vmem((levels + 1, ext, cols), F32),
            vmem((1, rows, cols), F32), vmem((1, rows, cols), F32),
            vmem((1, ext, cols), F32), vmem((1, ext, cols), F32),
            vmem((levels, ext, cols), F32),
            vmem((1, rows, cols), F32), vmem((1, rows, cols), F32),
            vmem((1, ext, cols), F32), vmem((1, ext, cols), F32),
            vmem((levels, rows, cols), F32),
            vmem((levels, 9 * cols, 2 * cols), BF16),
            vmem((2, levels, 2 * rows, ext), BF16),
            vmem((levels, members * ext, 6 * cols), BF16),
            vmem((levels, members * ext, 2 * cols), F32),
            vmem((ext, 2 * cols), F32),
            vmem((2, members, levels, rows, cols), F32),
            vmem((2, levels, rows, cols), F32),
            vmem((8, cols), F32),
            vmem((2, ext, cols), F32),
            vmem((levels, rows, cols), F32),
            vmem((2, n_mem - 1, rows, cols), F32),
            vmem((rows, cols), F32),
            vmem((2 * n_lat * n_mem, 8, cols), F32), vmem((n_lon // 2, 8, cols), F32),
        ]
        + [dma((6,))]
        + [dma((CHUNKS, 8))] * 2
        + [dma((8,))] * 4
        + [dma((n_mem - 1,))] * 4
        + [dma((n_mem - 1,))] * 2
        + [dma((2, n_mem))] * 2
        + [dma((n_mem - 1,))] * 4
        + [dma((2 * n_lat * n_mem - 1,))] * 2
        + [dma((n_lon // 2 - 1,))] * 2
        + [dma((4,))],
        compiler_params=pltpu.CompilerParams(
            collective_id=0, has_side_effects=True, vmem_limit_bytes=63 * 1024 * 1024
        ),
    )(
        band_width, anomalies, spread, obs_index.reshape(1, count), innovation.reshape(1, count),
        obs_weight.reshape(1, count),
    )
    return pl.pallas_call(
        combine,
        out_shape=(
            jax.ShapeDtypeStruct((members, levels, rows, cols), F32),
            jax.ShapeDtypeStruct((levels, rows, cols), F32),
        ),
        in_specs=[far] * 3,
        out_specs=(far, far),
        scratch_shapes=[
            vmem((2, members, levels, rows, cols), F32), vmem((2, levels, rows, cols), F32), vmem((8, cols), F32),
            dma((members,)), dma((2,)), dma((members + 1,)),
        ],
        compiler_params=pltpu.CompilerParams(vmem_limit_bytes=63 * 1024 * 1024),
    )(*done)


def solution(mesh):
    n_lon, n_lat, n_mem = (mesh.shape[name] for name in ("lon", "lat", "mem"))
    return jax.shard_map(
        lambda *args: per_device(n_lon, n_lat, n_mem, *args),
        mesh=mesh,
        in_specs=(
            P("mem", None, "lon", "lat"),
            P(None, "lon", "lat"),
            P("lon", "lat", None),
            P("lon", "lat", None),
            P("lon", "lat", None),
            P(),
        ),
        out_specs=(P("mem", None, "lon", "lat"), P(None, "lon", "lat")),
        check_vma=False,
    )
```

```python
import math

import jax
import jax.numpy as jnp
from jax import lax
from jax.experimental import pallas as pl
from jax.experimental.pallas import tpu as pltpu
from jax.sharding import PartitionSpec as P

BAND = 12
HALO = 2 * BAND
CHUNKS = 4
hybrid_ens = 0.75
hybrid_static = 0.25
F32, BF16 = jnp.float32, jnp.bfloat16
HI = lax.Precision.HIGHEST
MESH = pl.DeviceIdType.MESH
AROUND = [(dx, dy) for dy in (0, 1, -1) for dx in (1, -1, 0) if (dx, dy) != (0, 0)]


def iota(shape, axis):
    return lax.broadcasted_iota(jnp.int32, shape, axis)


def dot(a, b, precision=None):
    return jnp.dot(a, b, preferred_element_type=F32, precision=precision)


def split(x):
    high = x.astype(BF16)
    return high, (x - high.astype(F32)).astype(BF16)


def kernel(dims, band_any, a_any, s_any, idx_any, inn_any, wt_any, ens_out, static_out, lam_out,
           band_ref, idx_ref, inn_ref, wt_ref, ac, kl, kr, hl, hr, f0c, k0l, k0r, f0l, f0r, f1c, k1l, k1r, f1l, f1r,
           obs, mlat, nlon, nrim, xs, ub, us, p_ref, ps_ref, lam_ref, sl, y_ref, yr, t1_ref, gather_plane, gather_lon,
           in_sem, a_send, a_recv, f0_send, f0_recv, z_send, z_recv, f1_send, f1_recv, r0_send, r0_recv, r1_send, r1_recv,
           g_send, g_recv, c1_send, c1_recv, q0_send, q0_recv, q1_send, q1_recv, sp_send, sp_recv, so_send, so_recv, out_sem):
    n_lon, n_lat, n_mem, members, levels, rows, cols = dims
    lon, lat, mem = lax.axis_index("lon"), lax.axis_index("lat"), lax.axis_index("mem")
    ce2 = hybrid_ens / (members * n_mem)
    cs2 = hybrid_static
    ext = rows + 2 * HALO

    def at(dlon=0, dlat=0, dmem=0):
        return {
            "lon": lax.rem(lon + (dlon + n_lon), n_lon),
            "lat": lax.rem(lat + (dlat + n_lat), n_lat),
            "mem": lax.rem(mem + (dmem + n_mem), n_mem),
        }

    def copy(src, dst, send, recv, device):
        return pltpu.make_async_remote_copy(
            src_ref=src, dst_ref=dst, send_sem=send, recv_sem=recv, device_id=device, device_id_type=MESH
        )
    parity = lax.rem(lon, 2)
    across = 1 - 2 * parity
    plane = [(tx * across, ol, om) for tx in range(2) for ol in range(n_lat) for om in range(n_mem)][1:]
    line = [(o, 0, 0) for o in range(2, n_lon, 2)]
    partners = plane + line + [(-across, dy, 0) for dy in (0, 1, -1)] + [(-across, 0, o) for o in range(1, n_mem)]
    barrier = pltpu.get_barrier_semaphore()
    for partner in partners:
        pl.semaphore_signal(barrier, inc=1, device_id=at(*partner), device_id_type=MESH)

    own = pl.ds(0, rows)
    inputs = [
        pltpu.make_async_copy(src, dst, in_sem.at[number])
        for number, (src, dst) in enumerate((
            (a_any, ac.at[:, :, own, :]), (s_any.at[mem], f0c.at[levels, own, :]), (band_any, band_ref),
            (idx_any, idx_ref), (inn_any, inn_ref), (wt_any, wt_ref),
        ))
    ]
    for one in inputs:
        one.start()
    low, high = pl.ds(rows, HALO), pl.ds(rows + HALO, HALO)
    first, last = pl.ds(0, HALO), pl.ds(rows - HALO, HALO)
    sel_row, sel_col = iota((levels * cols, 2 * cols), 0), iota((levels * cols, 2 * cols), 1)
    sel_level, sel_lat = sel_row // cols, lax.rem(sel_row, cols)
    spot = lax.rem(sel_col, cols) - HALO * sel_level
    wanted = jnp.where(sel_col < cols, spot + (cols - HALO), spot)
    select = jnp.where((spot >= 0) & (spot < HALO) & (sel_lat == wanted), 1.0, 0.0)

    for one in inputs:
        one.wait()
    packed = dot(
        jnp.concatenate([ac[:, l, own, :].reshape(members * rows, cols) for l in range(levels)], axis=1),
        select.astype(BF16),
    ).astype(BF16)
    kl[...] = packed[:, :cols].reshape(members, rows, cols)
    kr[...] = packed[:, cols:].reshape(members, rows, cols)
    pl.semaphore_wait(barrier, len(partners))

    from_rows = {1: last, -1: first, 0: pl.ds(0, rows)}
    to_rows = {1: low, -1: high, 0: own}

    def halo(centre, left, right, packed_left, packed_right, send, recv, chunk=None, skip=0):
        copies = []
        for number, (dx, dy) in enumerate(AROUND[skip:]):
            if dy == 0:
                if chunk is None:
                    src, dst = centre.at[:, from_rows[dx], :], centre.at[:, to_rows[dx], :]
                else:
                    src, dst = centre.at[chunk, :, from_rows[dx], :], centre.at[chunk, :, to_rows[dx], :]
            else:
                every = slice(None) if chunk is None else chunk
                src = (packed_left if dy == 1 else packed_right).at[every, from_rows[dx], :]
                dst = (left if dy == 1 else right).at[every, to_rows[dx], :]
            one = copy(src, dst, send.at[number], recv.at[number], at(dx, dy))
            one.start()
            copies.append(one)
        return copies

    batch = members // CHUNKS

    def send_chunk(number):
        return halo(ac, hl, hr, kl, kr, a_send.at[number], a_recv.at[number], pl.ds(number * batch, batch))
    a_copies = [send_chunk(0)]
    index = idx_ref[...]
    weight = wt_ref[...]
    at_row, at_col = index // cols, lax.rem(index, cols)
    count = index.shape[1]
    columns = jnp.where(iota((cols, count), 0) == at_col, 1.0, 0.0).astype(BF16)

    def thirds(v):
        one = v.astype(BF16).astype(F32)
        two = (v - one).astype(BF16).astype(F32)
        return [one, two, v - one - two]

    terms = thirds(weight) + thirds(weight * inn_ref[...])

    def level_fields(l, carry):
        here = (iota((rows, count), 0) + rows * l) == at_row
        stacked = jnp.concatenate([jnp.where(here, t, 0.0).astype(BF16) for t in terms], axis=0)
        sums = lax.dot_general(stacked, columns, (((1,), (1,)), ((), ())), preferred_element_type=F32)
        obs[l] = sums[0:rows] + sums[rows:2 * rows] + sums[2 * rows:3 * rows]
        f0c[l, own, :] = sums[3 * rows:4 * rows] + sums[4 * rows:5 * rows] + sums[5 * rows:]
        return carry

    lax.fori_loop(0, levels, level_fields, 0)

    select16 = select.astype(BF16)

    def select_exact(x, chosen):
        terms = dot(jnp.concatenate([t.astype(BF16) for t in thirds(x)], axis=0), chosen)
        return terms[0:rows] + terms[rows:2 * rows] + terms[2 * rows:]

    def pack(centre, left, right, extra=0.0):
        whole = jnp.concatenate([centre[l, own, :] for l in range(levels)], axis=1)
        both = select_exact(whole, select16) + extra
        left[0] = both[:, :cols]
        right[0] = both[:, cols:]

    spare = levels * HALO
    spot = lax.rem(iota((cols, 2 * cols), 1), cols) - spare
    wanted = jnp.where(iota((cols, 2 * cols), 1) < cols, spot + (cols - HALO), spot)
    place = jnp.where((spot >= 0) & (spot < HALO) & (iota((cols, 2 * cols), 0) == wanted), 1.0, 0.0)
    pack(f0c, k0l, k0r, select_exact(f0c[levels, own, :], place.astype(BF16)))
    half = levels // 2
    ours = pl.ds(half * lax.rem(mem, 2), half)
    twin = 1 - 2 * lax.rem(mem, 2)
    z_copies, s_copies = [], []
    for number, dx in enumerate((1, -1)):
        for kind, (some, group) in enumerate(((ours, z_copies), (pl.ds(levels, 1), s_copies))):
            one = copy(
                f0c.at[some, from_rows[dx], :], f0c.at[some, to_rows[dx], :],
                z_send.at[2 * kind + number], z_recv.at[2 * kind + number], at(dx, 0, 0),
            )
            one.start()
            group.append(one)
    f0_copies = s_copies + halo(f0c, f0l, f0r, k0l, k0r, f0_send, f0_recv, skip=2)
    a_copies.append(send_chunk(1))
    r, c = iota((cols, cols), 0), iota((cols, cols), 1)
    inside_low = jnp.where(lat > 0, 1.0, 0.0).astype(F32)
    inside_high = jnp.where(lat < n_lat - 1, 1.0, 0.0).astype(F32)
    offsets = iota((8, cols), 1) - BAND

    def spot_of(row):
        return jnp.where(row < rows, row, jnp.where(row < rows + HALO, row - rows - HALO, row - HALO))

    def level_matrices(l, carry):
        def band_of(which):
            width = jnp.full((1, 1), band_ref[which, l].astype(F32), F32)

            def raw(diff):
                d = diff.astype(F32)
                ratio = d / (0.5 * width)
                return jnp.where(jnp.abs(d) <= width, jnp.exp(-0.5 * (ratio * ratio)), 0.0)

            total = jnp.sum(raw(offsets), axis=1, keepdims=True)[0:1]
            return lambda diff: raw(diff) / total

        band = band_of(1)
        spot = r - HALO * l
        valid = jnp.where((spot >= 0) & (spot < HALO), 1.0, 0.0)
        d0, dm, dp = band(r - c), band(r - cols - c), band(r + cols - c)
        from_low = spot + (cols - HALO)
        dml, d0l = band(from_low - cols - c) * valid, band(from_low - c) * valid
        dpr, d0r = band(spot + cols - c) * valid, band(spot - c) * valid
        twice = [
            dot(d0, d0, HI) + inside_low * dot(dp, dm, HI) + inside_high * dot(dm, dp, HI),
            inside_low * (dot(d0l, dm, HI) + dot(dml, d0, HI)),
            inside_high * (dot(d0r, dp, HI) + dot(dpr, d0, HI)),
        ]
        once = [d0, inside_low * dml, inside_high * dpr]
        for part in range(3):
            hi, lo = split(jnp.concatenate([twice[part], once[part]], axis=1))
            mlat[l, part * cols:(part + 1) * cols, :] = hi
            mlat[l, (3 + part) * cols:(4 + part) * cols, :] = hi
            mlat[l, (6 + part) * cols:(7 + part) * cols, :] = lo
        band = band_of(0)
        near = band(iota((rows, ext), 0) - spot_of(iota((rows, ext), 1)))
        far = band(spot_of(iota((ext, ext), 0)) - spot_of(iota((ext, ext), 1)))
        for which, matrix in enumerate((dot(near, far, HI), near)):
            hi, lo = split(matrix)
            nlon[which, l, 0:rows, :] = hi
            nlon[which, l, rows:2 * rows, :] = lo
            nrim[which, l, 0:rows, :] = hi[:, rows:]
            nrim[which, l, rows:2 * rows, :] = lo[:, rows:]
        return carry

    lax.fori_loop(0, levels, level_matrices, 0)
    a_copies.append(send_chunk(2))
    for number, (one, rim) in enumerate(zip(z_copies, (low, high))):
        one.wait_recv()
        passed = copy(
            f0c.at[ours, rim, :], f0c.at[ours, rim, :],
            z_send.at[4 + number], z_recv.at[4 + number], at(0, 0, twin),
        )
        passed.start()
        f0_copies.append(passed)
    for one in f0_copies:
        one.wait_recv()
    a_copies.append(send_chunk(3))
    realign = jnp.where((r - spare == c - HALO * mem) & (r >= spare) & (r < spare + HALO), 1.0, 0.0)
    sl[0] = dot(f0l[0], realign, HI)
    sl[1] = dot(f0r[0], realign, HI)

    def lon_pass(l, u_hi, u_lo, which, matrix=nlon):
        depth = u_hi.shape[0]
        both = matrix[which, l] if matrix.shape[3] == depth else matrix[which, l, :, 0:depth]
        tall = dot(both, u_hi)
        return tall[0:rows] + tall[rows:] + dot(both[0:rows], u_lo)

    every_row = (0, ext, 0)
    own_rows, rim_rows = (0, rows, 0), (rows, 2 * HALO, members * rows)

    def apply_members(centre, left, right, start, count, part, fresh):
        row, size, base = part
        some = pl.ds(row, size)
        zl, zr = left[0, some, :], right[0, some, :]
        z = [centre[l, some, :] for l in range(levels)]
        chunk = pl.ds(base + start * size, count * size)
        for k in range(start, start + count):
            spans = pl.ds(base + k * size, size)
            for side, (rim, zz) in enumerate(((hl, zl), (hr, zr))):
                hi, lo = split(rim[k, some, :].astype(F32) * zz)
                for l in range(levels):
                    xs[l, spans, (1 + side) * cols:(2 + side) * cols] = hi
                    xs[l, spans, (4 + side) * cols:(5 + side) * cols] = lo
            for l in range(levels):
                hi, lo = split(ac[k, l, some, :].astype(F32) * z[l])
                xs[l, spans, 0:cols] = hi
                xs[l, spans, 3 * cols:4 * cols] = lo
        for l in range(levels):
            ub[l, chunk, :] = dot(xs[l, chunk, :], mlat[l, 0:6 * cols, :]) + dot(
                xs[l, chunk, 0:3 * cols], mlat[l, 6 * cols:, :]
            )
        for l in range(levels):
            total = jnp.zeros((rows, cols), F32)
            for k in range(start, start + count):
                hi, lo = split(ub[l, pl.ds(base + k * size, size), 0:cols])
                part_sum = lon_pass(l, hi, lo, 0, nrim if row else nlon)
                total += ac[k, l, own, :].astype(F32) * part_sum
            y_ref[l] = ce2 * total if fresh else y_ref[l] + ce2 * total

    def apply_static(centre, left, right):
        his, los = [], []
        for stat, z in ((f0c[levels], centre[mem]), (sl[0], left[0]), (sl[1], right[0])):
            hi, lo = split(stat * z)
            his.append(hi)
            los.append(lo)
        u = dot(jnp.concatenate(his + los, axis=1), mlat[mem, 0:6 * cols, :])
        us[...] = u + dot(jnp.concatenate(his, axis=1), mlat[mem, 6 * cols:, :])
        hi, lo = split(us[:, 0:cols])
        y_ref[mem] = y_ref[mem] + cs2 * f0c[levels, own, :] * lon_pass(mem, hi, lo, 0)

    def parts(turn, which):
        for l in which:
            for k in range(members):
                if turn == 0:
                    u = ub[l, pl.ds(k * ext, ext), cols:2 * cols]
                else:
                    u = jnp.concatenate(
                        [ub[l, pl.ds(base + k * size, size), cols:2 * cols] for _, size, base in (own_rows, rim_rows)],
                        axis=0,
                    )
                hi, lo = split(u)
                p_ref[turn, k, l] = math.sqrt(ce2) * lon_pass(l, hi, lo, 1)

    def static_part(turn, send, recv):
        hi, lo = split(us[:, cols:2 * cols])
        ps_ref[turn, mem] = math.sqrt(cs2) * lon_pass(mem, hi, lo, 1)
        copies = []
        for o in range(1, n_mem):
            one = copy(
                ps_ref.at[turn, mem], ps_ref.at[turn, mem], send.at[o - 1], recv.at[o - 1], at(0, 0, o)
            )
            one.start()
            copies.append(one)
        return copies

    def scatter_sum(slots, send, recv):
        copies = []
        for o in range(1, n_mem):
            other = lax.rem(mem + o, n_mem)
            one = copy(y_ref.at[other], slots.at[o - 1], send.at[o - 1], recv.at[o - 1], at(0, 0, o))
            one.start()
            copies.append(one)
        return copies

    def finish_sum(copies, slots):
        total = y_ref[mem]
        for o, one in enumerate(copies):
            one.wait()
            total = total + slots[o]
        return total

    for number in range(CHUNKS):
        for one in a_copies[number]:
            one.wait_recv()
        apply_members(f0c, f0l, f0r, number * batch, batch, every_row, number == 0)
    r0_copies = scatter_sum(yr.at[0], r0_send, r0_recv)
    apply_static(f0c, f0l, f0r)
    parts(0, (0, 1))
    y0 = finish_sum(r0_copies, yr.at[0])
    t0 = f0c[mem, own, :]
    t1 = obs[mem] * y0
    t1_ref[...] = t1
    f1c[mem, own, :] = t1
    g_copies, c1_copies = [], []
    for o in range(1, n_mem):
        one = copy(t1_ref, f1c.at[mem, own, :], g_send.at[o - 1], g_recv.at[o - 1], at(0, 0, o))
        one.start()
        g_copies.append(one)
    parts(0, (2, 3))
    outs = [pltpu.make_async_copy(p_ref.at[0], ens_out.at[0], out_sem.at[0])]
    outs[-1].start()
    for one in g_copies:
        one.wait_recv()
    pack(f1c, k1l, k1r)
    f1_copies = halo(f1c, f1l, f1r, k1l, k1r, f1_send, f1_recv, skip=2)
    f1_lat = [one for one, (dx, dy) in zip(f1_copies, AROUND[2:]) if dx == 0]
    f1_corners = [one for one, (dx, dy) in zip(f1_copies, AROUND[2:]) if dx != 0]
    for number, dx in enumerate((1, -1)):
        for o in range(n_mem):
            one = copy(
                t1_ref.at[from_rows[dx], :], f1c.at[mem, to_rows[dx], :],
                c1_send.at[number, o], c1_recv.at[number, o], at(dx, 0, o),
            )
            one.start()
            c1_copies.append(one)
    for one in f1_lat:
        one.wait_recv()
    apply_members(f1c, f1l, f1r, 0, members, own_rows, True)
    for one in f1_corners + c1_copies:
        one.wait_recv()
    q0_copies = static_part(0, q0_send, q0_recv)
    apply_members(f1c, f1l, f1r, 0, members, rim_rows, False)
    r1_copies = scatter_sum(yr.at[1], r1_send, r1_recv)
    apply_static(f1c, f1l, f1r)
    parts(1, range(levels))
    outs.append(pltpu.make_async_copy(p_ref.at[1], ens_out.at[1], out_sem.at[1]))
    outs[-1].start()
    y1 = finish_sum(r1_copies, yr.at[1])

    def summed(x):
        return jnp.sum(jnp.sum(x, axis=0, keepdims=True), axis=1, keepdims=True)

    lane = iota((8, cols), 1)
    sums = jnp.zeros((8, cols), F32)
    for number, value in enumerate((t0 * y0, t1 * y0, t1 * y1, y1 * (obs[mem] * y1))):
        sums = jnp.where(lane == number, summed(value), sums)

    def total_start(value, slots, me, offsets, send, recv):
        slots[me] = value
        copies = []
        for number, offset in enumerate(offsets):
            one = copy(slots.at[me, 0:1, :], slots.at[me, 0:1, :], send.at[number], recv.at[number], at(*offset))
            one.start()
            copies.append(one)
        return copies

    def total_finish(slots, copies):
        for one in copies:
            one.wait_recv()
        out = slots[0, 0:1, :]
        for other in range(1, len(copies) + 1):
            out = out + slots[other, 0:1, :]
        return jnp.broadcast_to(out, (8, cols))

    plane_copies = total_start(sums, gather_plane, (parity * n_lat + lat) * n_mem + mem, plane, sp_send, sp_recv)
    sums = total_finish(gather_plane, plane_copies)
    line_copies = total_start(sums, gather_lon, lon // 2, line, so_send, so_recv)
    q1_copies = static_part(1, q1_send, q1_recv)
    sums = total_finish(gather_lon, line_copies)
    row = sums[0:1]

    def pick(number):
        return jnp.sum(jnp.where(iota((1, cols), 1) == number, row, 0.0), axis=1, keepdims=True)

    rr = pick(0)
    u, v, s = pick(1) / rr, pick(2) / rr, pick(3) / rr
    alpha = 1.0 / (1.0 + u)
    beta = (v - u * u) * alpha * alpha
    g, h = 1.0 - alpha + beta, -alpha
    alpha_next = beta / (g * g * (1.0 + u) + 2.0 * g * h * (u + v) + h * h * (v + s))
    lam_ref[...] = jnp.where(lane == 0, alpha + alpha_next * g, alpha_next * h)
    outs.append(pltpu.make_async_copy(lam_ref, lam_out, out_sem.at[2]))
    outs[-1].start()
    for one in q0_copies + q1_copies:
        one.wait()
    outs.append(pltpu.make_async_copy(ps_ref, static_out, out_sem.at[3]))
    outs[-1].start()
    for one in outs:
        one.wait()
    for copies in a_copies:
        for one in copies:
            one.wait_send()
    for one in z_copies + f0_copies + g_copies + c1_copies + f1_copies + plane_copies + line_copies:
        one.wait_send()


def combine(ens_in, static_in, lam_in, ens_out, static_out, ens, static, lam, ens_sem, in_sem, out_sem):
    members = ens_out.shape[0]
    lam_copy = pltpu.make_async_copy(lam_in, lam, in_sem.at[0])
    static_copy = pltpu.make_async_copy(static_in, static, in_sem.at[1])
    lam_copy.start()
    loads = [pltpu.make_async_copy(ens_in.at[:, k], ens.at[:, k], ens_sem.at[k]) for k in range(members)]
    for one in loads:
        one.start()
    static_copy.start()
    lam_copy.wait()
    near, far = lam[0:1, 0:1], lam[0:1, 1:2]
    stores = []
    for k in range(members):
        loads[k].wait()
        ens[0, k] = near * ens[0, k] + far * ens[1, k]
        stores.append(pltpu.make_async_copy(ens.at[0, k], ens_out.at[k], out_sem.at[k]))
        stores[-1].start()
    static_copy.wait()
    static[0] = near * static[0] + far * static[1]
    stores.append(pltpu.make_async_copy(static.at[0], static_out, out_sem.at[members]))
    stores[-1].start()
    for one in stores:
        one.wait()


def per_device(n_lon, n_lat, n_mem, anomalies, spread, obs_index, innovation, obs_weight, band_width):
    members, levels, rows, cols = anomalies.shape
    ext = rows + 2 * HALO
    count = obs_index.shape[-1]
    vmem, dma = pltpu.VMEM, pltpu.SemaphoreType.DMA
    dims = (n_lon, n_lat, n_mem, members, levels, rows, cols)
    far = pl.BlockSpec(memory_space=pltpu.HBM)
    done = pl.pallas_call(
        lambda *refs: kernel(dims, *refs),
        out_shape=(
            jax.ShapeDtypeStruct((2, members, levels, rows, cols), F32),
            jax.ShapeDtypeStruct((2, levels, rows, cols), F32),
            jax.ShapeDtypeStruct((8, cols), F32),
        ),
        in_specs=[far] * 6,
        out_specs=(far, far, far),
        scratch_shapes=[
            pltpu.SMEM((2, levels), jnp.int32),
            vmem((1, count), jnp.int32), vmem((1, count), F32), vmem((1, count), F32),
            vmem((members, levels, ext, cols), BF16),
            vmem((members, rows, cols), BF16), vmem((members, rows, cols), BF16),
            vmem((members, ext, cols), BF16), vmem((members, ext, cols), BF16),
            vmem((levels + 1, ext, cols), F32),
            vmem((1, rows, cols), F32), vmem((1, rows, cols), F32),
            vmem((1, ext, cols), F32), vmem((1, ext, cols), F32),
            vmem((levels, ext, cols), F32),
            vmem((1, rows, cols), F32), vmem((1, rows, cols), F32),
            vmem((1, ext, cols), F32), vmem((1, ext, cols), F32),
            vmem((levels, rows, cols), F32),
            vmem((levels, 9 * cols, 2 * cols), BF16),
            vmem((2, levels, 2 * rows, ext), BF16),
            vmem((2, levels, 2 * rows, 2 * HALO), BF16),
            vmem((levels, members * ext, 6 * cols), BF16),
            vmem((levels, members * ext, 2 * cols), F32),
            vmem((ext, 2 * cols), F32),
            vmem((2, members, levels, rows, cols), F32),
            vmem((2, levels, rows, cols), F32),
            vmem((8, cols), F32),
            vmem((2, ext, cols), F32),
            vmem((levels, rows, cols), F32),
            vmem((2, n_mem - 1, rows, cols), F32),
            vmem((rows, cols), F32),
            vmem((2 * n_lat * n_mem, 8, cols), F32), vmem((n_lon // 2, 8, cols), F32),
        ]
        + [dma((6,))]
        + [dma((CHUNKS, 8))] * 2
        + [dma((8,))] * 2
        + [dma((6,))] * 2
        + [dma((8,))] * 2
        + [dma((n_mem - 1,))] * 4
        + [dma((n_mem - 1,))] * 2
        + [dma((2, n_mem))] * 2
        + [dma((n_mem - 1,))] * 4
        + [dma((2 * n_lat * n_mem - 1,))] * 2
        + [dma((n_lon // 2 - 1,))] * 2
        + [dma((4,))],
        compiler_params=pltpu.CompilerParams(
            collective_id=0, has_side_effects=True, vmem_limit_bytes=63 * 1024 * 1024
        ),
    )(
        band_width, anomalies, spread, obs_index.reshape(1, count), innovation.reshape(1, count),
        obs_weight.reshape(1, count),
    )
    return pl.pallas_call(
        combine,
        out_shape=(
            jax.ShapeDtypeStruct((members, levels, rows, cols), F32),
            jax.ShapeDtypeStruct((levels, rows, cols), F32),
        ),
        in_specs=[far] * 3,
        out_specs=(far, far),
        scratch_shapes=[
            vmem((2, members, levels, rows, cols), F32), vmem((2, levels, rows, cols), F32), vmem((8, cols), F32),
            dma((members,)), dma((2,)), dma((members + 1,)),
        ],
        compiler_params=pltpu.CompilerParams(vmem_limit_bytes=63 * 1024 * 1024),
    )(*done)


def solution(mesh):
    n_lon, n_lat, n_mem = (mesh.shape[name] for name in ("lon", "lat", "mem"))
    return jax.shard_map(
        lambda *args: per_device(n_lon, n_lat, n_mem, *args),
        mesh=mesh,
        in_specs=(
            P("mem", None, "lon", "lat"),
            P(None, "lon", "lat"),
            P("lon", "lat", None),
            P("lon", "lat", None),
            P("lon", "lat", None),
            P(),
        ),
        out_specs=(P("mem", None, "lon", "lat"), P(None, "lon", "lat")),
        check_vma=False,
    )
```

```python
import math

import jax
import jax.numpy as jnp
from jax import lax
from jax.experimental import pallas as pl
from jax.experimental.pallas import tpu as pltpu
from jax.sharding import PartitionSpec as P

BAND = 12
HALO = 2 * BAND
CHUNKS = 4
hybrid_ens = 0.75
hybrid_static = 0.25
F32, BF16 = jnp.float32, jnp.bfloat16
HI = lax.Precision.HIGHEST
MESH = pl.DeviceIdType.MESH
AROUND = [(dx, dy) for dy in (0, 1, -1) for dx in (1, -1, 0) if (dx, dy) != (0, 0)]


def iota(shape, axis):
    return lax.broadcasted_iota(jnp.int32, shape, axis)


def dot(a, b, precision=None):
    return jnp.dot(a, b, preferred_element_type=F32, precision=precision)


def split(x):
    high = x.astype(BF16)
    return high, (x - high.astype(F32)).astype(BF16)


def kernel(dims, band_any, a_any, s_any, idx_any, inn_any, wt_any, ens_out, static_out, lam_out,
           band_ref, idx_ref, inn_ref, wt_ref, ac, kl, kr, hl, hr, f0c, k0l, k0r, f0l, f0r, f1c, k1l, k1r, f1l, f1r,
           obs, mlat, nlon, nrim, xs, ub, us, p_ref, ps_ref, lam_ref, sl, y_ref, yr, t1_ref, gather_plane, gather_lon,
           in_sem, a_send, a_recv, f0_send, f0_recv, z_send, z_recv, f1_send, f1_recv, r0_send, r0_recv, r1_send, r1_recv,
           g_send, g_recv, c1_send, c1_recv, q0_send, q0_recv, q1_send, q1_recv, sp_send, sp_recv, so_send, so_recv, out_sem):
    n_lon, n_lat, n_mem, members, levels, rows, cols = dims
    lon, lat, mem = lax.axis_index("lon"), lax.axis_index("lat"), lax.axis_index("mem")
    ce2 = hybrid_ens / (members * n_mem)
    cs2 = hybrid_static
    ext = rows + 2 * HALO

    def at(dlon=0, dlat=0, dmem=0):
        return {
            "lon": lax.rem(lon + (dlon + n_lon), n_lon),
            "lat": lax.rem(lat + (dlat + n_lat), n_lat),
            "mem": lax.rem(mem + (dmem + n_mem), n_mem),
        }

    def copy(src, dst, send, recv, device):
        return pltpu.make_async_remote_copy(
            src_ref=src, dst_ref=dst, send_sem=send, recv_sem=recv, device_id=device, device_id_type=MESH
        )
    parity = lax.rem(lon, 2)
    across = 1 - 2 * parity
    plane = [(tx * across, ol, om) for tx in range(2) for ol in range(n_lat) for om in range(n_mem)][1:]
    line = [(o, 0, 0) for o in range(2, n_lon, 2)]
    partners = plane + line + [(-across, dy, 0) for dy in (0, 1, -1)] + [(-across, 0, o) for o in range(1, n_mem)]
    barrier = pltpu.get_barrier_semaphore()
    for partner in partners:
        pl.semaphore_signal(barrier, inc=1, device_id=at(*partner), device_id_type=MESH)

    own = pl.ds(0, rows)
    inputs = [
        pltpu.make_async_copy(src, dst, in_sem.at[number])
        for number, (src, dst) in enumerate((
            (a_any, ac.at[:, :, own, :]), (s_any.at[mem], f0c.at[levels, own, :]), (band_any, band_ref),
            (idx_any, idx_ref), (inn_any, inn_ref), (wt_any, wt_ref),
        ))
    ]
    for one in inputs:
        one.start()
    low, high = pl.ds(rows, HALO), pl.ds(rows + HALO, HALO)
    first, last = pl.ds(0, HALO), pl.ds(rows - HALO, HALO)
    sel_row, sel_col = iota((levels * cols, 2 * cols), 0), iota((levels * cols, 2 * cols), 1)
    sel_level, sel_lat = sel_row // cols, lax.rem(sel_row, cols)
    spot = lax.rem(sel_col, cols) - HALO * sel_level
    wanted = jnp.where(sel_col < cols, spot + (cols - HALO), spot)
    select = jnp.where((spot >= 0) & (spot < HALO) & (sel_lat == wanted), 1.0, 0.0)

    for one in inputs:
        one.wait()
    packed = dot(
        jnp.concatenate([ac[:, l, own, :].reshape(members * rows, cols) for l in range(levels)], axis=1),
        select.astype(BF16),
    ).astype(BF16)
    kl[...] = packed[:, :cols].reshape(members, rows, cols)
    kr[...] = packed[:, cols:].reshape(members, rows, cols)
    pl.semaphore_wait(barrier, len(partners))

    from_rows = {1: last, -1: first, 0: pl.ds(0, rows)}
    to_rows = {1: low, -1: high, 0: own}

    def halo(centre, left, right, packed_left, packed_right, send, recv, chunk=None, takes=lambda dx, dy: True):
        copies = []
        for number, (dx, dy) in enumerate(AROUND):
            if not takes(dx, dy):
                continue
            if dy == 0:
                if chunk is None:
                    src, dst = centre.at[:, from_rows[dx], :], centre.at[:, to_rows[dx], :]
                else:
                    src, dst = centre.at[chunk, :, from_rows[dx], :], centre.at[chunk, :, to_rows[dx], :]
            else:
                every = slice(None) if chunk is None else chunk
                src = (packed_left if dy == 1 else packed_right).at[every, from_rows[dx], :]
                dst = (left if dy == 1 else right).at[every, to_rows[dx], :]
            one = copy(src, dst, send.at[number], recv.at[number], at(dx, dy))
            one.start()
            copies.append(one)
        return copies

    batch = members // CHUNKS

    def send_chunk(number):
        return halo(
            ac, hl, hr, kl, kr, a_send.at[number], a_recv.at[number], pl.ds(number * batch, batch),
            lambda dx, dy: dx != 0,
        )
    a_copies = [send_chunk(0)]
    a_lat = halo(
        ac, hl, hr, kl, kr, a_send.at[0], a_recv.at[0], pl.ds(0, members), lambda dx, dy: dx == 0
    )
    index = idx_ref[...]
    weight = wt_ref[...]
    at_row, at_col = index // cols, lax.rem(index, cols)
    count = index.shape[1]
    columns = jnp.where(iota((cols, count), 0) == at_col, 1.0, 0.0).astype(BF16)

    def thirds(v):
        one = v.astype(BF16).astype(F32)
        two = (v - one).astype(BF16).astype(F32)
        return [one, two, v - one - two]

    terms = thirds(weight) + thirds(weight * inn_ref[...])

    def level_fields(l, carry):
        here = (iota((rows, count), 0) + rows * l) == at_row
        stacked = jnp.concatenate([jnp.where(here, t, 0.0).astype(BF16) for t in terms], axis=0)
        sums = lax.dot_general(stacked, columns, (((1,), (1,)), ((), ())), preferred_element_type=F32)
        obs[l] = sums[0:rows] + sums[rows:2 * rows] + sums[2 * rows:3 * rows]
        f0c[l, own, :] = sums[3 * rows:4 * rows] + sums[4 * rows:5 * rows] + sums[5 * rows:]
        return carry

    lax.fori_loop(0, levels, level_fields, 0)

    select16 = select.astype(BF16)

    def select_exact(x, chosen):
        terms = dot(jnp.concatenate([t.astype(BF16) for t in thirds(x)], axis=0), chosen)
        return terms[0:rows] + terms[rows:2 * rows] + terms[2 * rows:]

    def pack(centre, left, right, extra=0.0):
        whole = jnp.concatenate([centre[l, own, :] for l in range(levels)], axis=1)
        both = select_exact(whole, select16) + extra
        left[0] = both[:, :cols]
        right[0] = both[:, cols:]

    spare = levels * HALO
    spot = lax.rem(iota((cols, 2 * cols), 1), cols) - spare
    wanted = jnp.where(iota((cols, 2 * cols), 1) < cols, spot + (cols - HALO), spot)
    place = jnp.where((spot >= 0) & (spot < HALO) & (iota((cols, 2 * cols), 0) == wanted), 1.0, 0.0)
    pack(f0c, k0l, k0r, select_exact(f0c[levels, own, :], place.astype(BF16)))
    half = levels // 2
    ours = pl.ds(half * lax.rem(mem, 2), half)
    twin = 1 - 2 * lax.rem(mem, 2)
    z_copies, s_copies = [], []
    for number, dx in enumerate((1, -1)):
        for kind, (some, group) in enumerate(((ours, z_copies), (pl.ds(levels, 1), s_copies))):
            one = copy(
                f0c.at[some, from_rows[dx], :], f0c.at[some, to_rows[dx], :],
                z_send.at[2 * kind + number], z_recv.at[2 * kind + number], at(dx, 0, 0),
            )
            one.start()
            group.append(one)
    f0_lat = halo(f0c, f0l, f0r, k0l, k0r, f0_send, f0_recv, takes=lambda dx, dy: dx == 0)
    f0_copies = s_copies + halo(
        f0c, f0l, f0r, k0l, k0r, f0_send, f0_recv, takes=lambda dx, dy: dx != 0 and dy != 0
    )
    a_copies.append(send_chunk(1))
    r, c = iota((cols, cols), 0), iota((cols, cols), 1)
    inside_low = jnp.where(lat > 0, 1.0, 0.0).astype(F32)
    inside_high = jnp.where(lat < n_lat - 1, 1.0, 0.0).astype(F32)
    offsets = iota((8, cols), 1) - BAND

    def spot_of(row):
        return jnp.where(row < rows, row, jnp.where(row < rows + HALO, row - rows - HALO, row - HALO))

    def level_matrices(l, carry):
        def band_of(which):
            width = jnp.full((1, 1), band_ref[which, l].astype(F32), F32)

            def raw(diff):
                d = diff.astype(F32)
                ratio = d / (0.5 * width)
                return jnp.where(jnp.abs(d) <= width, jnp.exp(-0.5 * (ratio * ratio)), 0.0)

            total = jnp.sum(raw(offsets), axis=1, keepdims=True)[0:1]
            return lambda diff: raw(diff) / total

        band = band_of(1)
        spot = r - HALO * l
        valid = jnp.where((spot >= 0) & (spot < HALO), 1.0, 0.0)
        d0, dm, dp = band(r - c), band(r - cols - c), band(r + cols - c)
        from_low = spot + (cols - HALO)
        dml, d0l = band(from_low - cols - c) * valid, band(from_low - c) * valid
        dpr, d0r = band(spot + cols - c) * valid, band(spot - c) * valid
        twice = [
            dot(d0, d0, HI) + inside_low * dot(dp, dm, HI) + inside_high * dot(dm, dp, HI),
            inside_low * (dot(d0l, dm, HI) + dot(dml, d0, HI)),
            inside_high * (dot(d0r, dp, HI) + dot(dpr, d0, HI)),
        ]
        once = [d0, inside_low * dml, inside_high * dpr]
        for part in range(3):
            hi, lo = split(jnp.concatenate([twice[part], once[part]], axis=1))
            mlat[l, part * cols:(part + 1) * cols, :] = hi
            mlat[l, (3 + part) * cols:(4 + part) * cols, :] = hi
            mlat[l, (6 + part) * cols:(7 + part) * cols, :] = lo
        band = band_of(0)
        near = band(iota((rows, ext), 0) - spot_of(iota((rows, ext), 1)))
        far = band(spot_of(iota((ext, ext), 0)) - spot_of(iota((ext, ext), 1)))
        for which, matrix in enumerate((dot(near, far, HI), near)):
            hi, lo = split(matrix)
            nlon[which, l, 0:rows, :] = hi
            nlon[which, l, rows:2 * rows, :] = lo
            nrim[which, l, 0:rows, :] = hi[:, rows:]
            nrim[which, l, rows:2 * rows, :] = lo[:, rows:]
        return carry

    lax.fori_loop(0, levels, level_matrices, 0)
    a_copies.append(send_chunk(2))
    def lon_pass(l, u_hi, u_lo, which, matrix=nlon):
        depth = u_hi.shape[0]
        both = matrix[which, l] if matrix.shape[3] == depth else matrix[which, l, :, 0:depth]
        tall = dot(both, u_hi)
        return tall[0:rows] + tall[rows:] + dot(both[0:rows], u_lo)

    own_rows, rim_rows = (0, rows, 0), (rows, 2 * HALO, members * rows)

    def apply_members(centre, left, right, start, count, part, fresh):
        row, size, base = part
        some = pl.ds(row, size)
        zl, zr = left[0, some, :], right[0, some, :]
        z = [centre[l, some, :] for l in range(levels)]
        chunk = pl.ds(base + start * size, count * size)
        for k in range(start, start + count):
            spans = pl.ds(base + k * size, size)
            for side, (rim, zz) in enumerate(((hl, zl), (hr, zr))):
                hi, lo = split(rim[k, some, :].astype(F32) * zz)
                for l in range(levels):
                    xs[l, spans, (1 + side) * cols:(2 + side) * cols] = hi
                    xs[l, spans, (4 + side) * cols:(5 + side) * cols] = lo
            for l in range(levels):
                hi, lo = split(ac[k, l, some, :].astype(F32) * z[l])
                xs[l, spans, 0:cols] = hi
                xs[l, spans, 3 * cols:4 * cols] = lo
        for l in range(levels):
            ub[l, chunk, :] = dot(xs[l, chunk, :], mlat[l, 0:6 * cols, :]) + dot(
                xs[l, chunk, 0:3 * cols], mlat[l, 6 * cols:, :]
            )
        for l in range(levels):
            total = jnp.zeros((rows, cols), F32)
            for k in range(start, start + count):
                hi, lo = split(ub[l, pl.ds(base + k * size, size), 0:cols])
                part_sum = lon_pass(l, hi, lo, 0, nrim if row else nlon)
                total += ac[k, l, own, :].astype(F32) * part_sum
            y_ref[l] = ce2 * total if fresh else y_ref[l] + ce2 * total

    def apply_static(centre, left, right):
        his, los = [], []
        for stat, z in ((f0c[levels], centre[mem]), (sl[0], left[0]), (sl[1], right[0])):
            hi, lo = split(stat * z)
            his.append(hi)
            los.append(lo)
        u = dot(jnp.concatenate(his + los, axis=1), mlat[mem, 0:6 * cols, :])
        us[...] = u + dot(jnp.concatenate(his, axis=1), mlat[mem, 6 * cols:, :])
        hi, lo = split(us[:, 0:cols])
        y_ref[mem] = y_ref[mem] + cs2 * f0c[levels, own, :] * lon_pass(mem, hi, lo, 0)

    def parts(turn, which):
        for l in which:
            for k in range(members):
                u = jnp.concatenate(
                    [ub[l, pl.ds(base + k * size, size), cols:2 * cols] for _, size, base in (own_rows, rim_rows)],
                    axis=0,
                )
                hi, lo = split(u)
                p_ref[turn, k, l] = math.sqrt(ce2) * lon_pass(l, hi, lo, 1)

    def static_part(turn, send, recv):
        hi, lo = split(us[:, cols:2 * cols])
        ps_ref[turn, mem] = math.sqrt(cs2) * lon_pass(mem, hi, lo, 1)
        copies = []
        for o in range(1, n_mem):
            one = copy(
                ps_ref.at[turn, mem], ps_ref.at[turn, mem], send.at[o - 1], recv.at[o - 1], at(0, 0, o)
            )
            one.start()
            copies.append(one)
        return copies

    def scatter_sum(slots, send, recv):
        copies = []
        for o in range(1, n_mem):
            other = lax.rem(mem + o, n_mem)
            one = copy(y_ref.at[other], slots.at[o - 1], send.at[o - 1], recv.at[o - 1], at(0, 0, o))
            one.start()
            copies.append(one)
        return copies

    def finish_sum(copies, slots):
        total = y_ref[mem]
        for o, one in enumerate(copies):
            one.wait()
            total = total + slots[o]
        return total

    for one in a_lat + f0_lat:
        one.wait_recv()
    apply_members(f0c, f0l, f0r, 0, members, own_rows, True)
    for number, (one, rim) in enumerate(zip(z_copies, (low, high))):
        one.wait_recv()
        passed = copy(
            f0c.at[ours, rim, :], f0c.at[ours, rim, :],
            z_send.at[4 + number], z_recv.at[4 + number], at(0, 0, twin),
        )
        passed.start()
        f0_copies.append(passed)
    a_copies.append(send_chunk(3))
    for one in f0_copies:
        one.wait_recv()
    realign = jnp.where((r - spare == c - HALO * mem) & (r >= spare) & (r < spare + HALO), 1.0, 0.0)
    sl[0] = dot(f0l[0], realign, HI)
    sl[1] = dot(f0r[0], realign, HI)

    for number in range(CHUNKS):
        for one in a_copies[number]:
            one.wait_recv()
        apply_members(f0c, f0l, f0r, number * batch, batch, rim_rows, False)
    r0_copies = scatter_sum(yr.at[0], r0_send, r0_recv)
    apply_static(f0c, f0l, f0r)
    parts(0, (0, 1))
    y0 = finish_sum(r0_copies, yr.at[0])
    t0 = f0c[mem, own, :]
    t1 = obs[mem] * y0
    t1_ref[...] = t1
    f1c[mem, own, :] = t1
    g_copies, c1_copies = [], []
    for o in range(1, n_mem):
        one = copy(t1_ref, f1c.at[mem, own, :], g_send.at[o - 1], g_recv.at[o - 1], at(0, 0, o))
        one.start()
        g_copies.append(one)
    parts(0, (2, 3))
    outs = [pltpu.make_async_copy(p_ref.at[0], ens_out.at[0], out_sem.at[0])]
    outs[-1].start()
    for one in g_copies:
        one.wait_recv()
    pack(f1c, k1l, k1r)
    f1_lat = halo(f1c, f1l, f1r, k1l, k1r, f1_send, f1_recv, takes=lambda dx, dy: dx == 0)
    f1_corners = halo(f1c, f1l, f1r, k1l, k1r, f1_send, f1_recv, takes=lambda dx, dy: dx != 0 and dy != 0)
    for number, dx in enumerate((1, -1)):
        for o in range(n_mem):
            one = copy(
                t1_ref.at[from_rows[dx], :], f1c.at[mem, to_rows[dx], :],
                c1_send.at[number, o], c1_recv.at[number, o], at(dx, 0, o),
            )
            one.start()
            c1_copies.append(one)
    for one in f1_lat:
        one.wait_recv()
    apply_members(f1c, f1l, f1r, 0, members, own_rows, True)
    for one in f1_corners + c1_copies:
        one.wait_recv()
    q0_copies = static_part(0, q0_send, q0_recv)
    apply_members(f1c, f1l, f1r, 0, members, rim_rows, False)
    r1_copies = scatter_sum(yr.at[1], r1_send, r1_recv)
    apply_static(f1c, f1l, f1r)
    parts(1, range(levels))
    outs.append(pltpu.make_async_copy(p_ref.at[1], ens_out.at[1], out_sem.at[1]))
    outs[-1].start()
    y1 = finish_sum(r1_copies, yr.at[1])

    def summed(x):
        return jnp.sum(jnp.sum(x, axis=0, keepdims=True), axis=1, keepdims=True)

    lane = iota((8, cols), 1)
    sums = jnp.zeros((8, cols), F32)
    for number, value in enumerate((t0 * y0, t1 * y0, t1 * y1, y1 * (obs[mem] * y1))):
        sums = jnp.where(lane == number, summed(value), sums)

    def total_start(value, slots, me, offsets, send, recv):
        slots[me] = value
        copies = []
        for number, offset in enumerate(offsets):
            one = copy(slots.at[me, 0:1, :], slots.at[me, 0:1, :], send.at[number], recv.at[number], at(*offset))
            one.start()
            copies.append(one)
        return copies

    def total_finish(slots, copies):
        for one in copies:
            one.wait_recv()
        out = slots[0, 0:1, :]
        for other in range(1, len(copies) + 1):
            out = out + slots[other, 0:1, :]
        return jnp.broadcast_to(out, (8, cols))

    plane_copies = total_start(sums, gather_plane, (parity * n_lat + lat) * n_mem + mem, plane, sp_send, sp_recv)
    sums = total_finish(gather_plane, plane_copies)
    line_copies = total_start(sums, gather_lon, lon // 2, line, so_send, so_recv)
    q1_copies = static_part(1, q1_send, q1_recv)
    for one in q0_copies + q1_copies:
        one.wait()
    outs.append(pltpu.make_async_copy(ps_ref, static_out, out_sem.at[3]))
    outs[-1].start()
    sums = total_finish(gather_lon, line_copies)
    row = sums[0:1]

    def pick(number):
        return jnp.sum(jnp.where(iota((1, cols), 1) == number, row, 0.0), axis=1, keepdims=True)

    rr = pick(0)
    u, v, s = pick(1) / rr, pick(2) / rr, pick(3) / rr
    alpha = 1.0 / (1.0 + u)
    beta = (v - u * u) * alpha * alpha
    g, h = 1.0 - alpha + beta, -alpha
    alpha_next = beta / (g * g * (1.0 + u) + 2.0 * g * h * (u + v) + h * h * (v + s))
    lam_ref[...] = jnp.where(lane == 0, alpha + alpha_next * g, alpha_next * h)
    outs.append(pltpu.make_async_copy(lam_ref, lam_out, out_sem.at[2]))
    outs[-1].start()
    for one in outs:
        one.wait()
    for copies in a_copies:
        for one in copies:
            one.wait_send()
    for one in z_copies + f0_lat + f0_copies + g_copies + c1_copies + f1_lat + f1_corners + a_lat + plane_copies + line_copies:
        one.wait_send()


def combine(ens_in, static_in, lam_in, ens_out, static_out, ens, static, lam, ens_sem, in_sem, out_sem):
    members = ens_out.shape[0]
    lam_copy = pltpu.make_async_copy(lam_in, lam, in_sem.at[0])
    static_copy = pltpu.make_async_copy(static_in, static, in_sem.at[1])
    lam_copy.start()
    loads = [pltpu.make_async_copy(ens_in.at[:, k], ens.at[:, k], ens_sem.at[k]) for k in range(members)]
    for one in loads:
        one.start()
    static_copy.start()
    lam_copy.wait()
    near, far = lam[0:1, 0:1], lam[0:1, 1:2]
    stores = []
    for k in range(members):
        loads[k].wait()
        ens[0, k] = near * ens[0, k] + far * ens[1, k]
        stores.append(pltpu.make_async_copy(ens.at[0, k], ens_out.at[k], out_sem.at[k]))
        stores[-1].start()
    static_copy.wait()
    static[0] = near * static[0] + far * static[1]
    stores.append(pltpu.make_async_copy(static.at[0], static_out, out_sem.at[members]))
    stores[-1].start()
    for one in stores:
        one.wait()


def per_device(n_lon, n_lat, n_mem, anomalies, spread, obs_index, innovation, obs_weight, band_width):
    members, levels, rows, cols = anomalies.shape
    ext = rows + 2 * HALO
    count = obs_index.shape[-1]
    vmem, dma = pltpu.VMEM, pltpu.SemaphoreType.DMA
    dims = (n_lon, n_lat, n_mem, members, levels, rows, cols)
    far = pl.BlockSpec(memory_space=pltpu.HBM)
    done = pl.pallas_call(
        lambda *refs: kernel(dims, *refs),
        out_shape=(
            jax.ShapeDtypeStruct((2, members, levels, rows, cols), F32),
            jax.ShapeDtypeStruct((2, levels, rows, cols), F32),
            jax.ShapeDtypeStruct((8, cols), F32),
        ),
        in_specs=[far] * 6,
        out_specs=(far, far, far),
        scratch_shapes=[
            pltpu.SMEM((2, levels), jnp.int32),
            vmem((1, count), jnp.int32), vmem((1, count), F32), vmem((1, count), F32),
            vmem((members, levels, ext, cols), BF16),
            vmem((members, rows, cols), BF16), vmem((members, rows, cols), BF16),
            vmem((members, ext, cols), BF16), vmem((members, ext, cols), BF16),
            vmem((levels + 1, ext, cols), F32),
            vmem((1, rows, cols), F32), vmem((1, rows, cols), F32),
            vmem((1, ext, cols), F32), vmem((1, ext, cols), F32),
            vmem((levels, ext, cols), F32),
            vmem((1, rows, cols), F32), vmem((1, rows, cols), F32),
            vmem((1, ext, cols), F32), vmem((1, ext, cols), F32),
            vmem((levels, rows, cols), F32),
            vmem((levels, 9 * cols, 2 * cols), BF16),
            vmem((2, levels, 2 * rows, ext), BF16),
            vmem((2, levels, 2 * rows, 2 * HALO), BF16),
            vmem((levels, members * ext, 6 * cols), BF16),
            vmem((levels, members * ext, 2 * cols), F32),
            vmem((ext, 2 * cols), F32),
            vmem((2, members, levels, rows, cols), F32),
            vmem((2, levels, rows, cols), F32),
            vmem((8, cols), F32),
            vmem((2, ext, cols), F32),
            vmem((levels, rows, cols), F32),
            vmem((2, n_mem - 1, rows, cols), F32),
            vmem((rows, cols), F32),
            vmem((2 * n_lat * n_mem, 8, cols), F32), vmem((n_lon // 2, 8, cols), F32),
        ]
        + [dma((6,))]
        + [dma((CHUNKS, 8))] * 2
        + [dma((8,))] * 2
        + [dma((6,))] * 2
        + [dma((8,))] * 2
        + [dma((n_mem - 1,))] * 4
        + [dma((n_mem - 1,))] * 2
        + [dma((2, n_mem))] * 2
        + [dma((n_mem - 1,))] * 4
        + [dma((2 * n_lat * n_mem - 1,))] * 2
        + [dma((n_lon // 2 - 1,))] * 2
        + [dma((4,))],
        compiler_params=pltpu.CompilerParams(
            collective_id=0, has_side_effects=True, vmem_limit_bytes=63 * 1024 * 1024
        ),
    )(
        band_width, anomalies, spread, obs_index.reshape(1, count), innovation.reshape(1, count),
        obs_weight.reshape(1, count),
    )
    return pl.pallas_call(
        combine,
        out_shape=(
            jax.ShapeDtypeStruct((members, levels, rows, cols), F32),
            jax.ShapeDtypeStruct((levels, rows, cols), F32),
        ),
        in_specs=[far] * 3,
        out_specs=(far, far),
        scratch_shapes=[
            vmem((2, members, levels, rows, cols), F32), vmem((2, levels, rows, cols), F32), vmem((8, cols), F32),
            dma((members,)), dma((2,)), dma((members + 1,)),
        ],
        compiler_params=pltpu.CompilerParams(vmem_limit_bytes=63 * 1024 * 1024),
    )(*done)


def solution(mesh):
    n_lon, n_lat, n_mem = (mesh.shape[name] for name in ("lon", "lat", "mem"))
    return jax.shard_map(
        lambda *args: per_device(n_lon, n_lat, n_mem, *args),
        mesh=mesh,
        in_specs=(
            P("mem", None, "lon", "lat"),
            P(None, "lon", "lat"),
            P("lon", "lat", None),
            P("lon", "lat", None),
            P("lon", "lat", None),
            P(),
        ),
        out_specs=(P("mem", None, "lon", "lat"), P(None, "lon", "lat")),
        check_vma=False,
    )
```

```python
import math

import jax
import jax.numpy as jnp
from jax import lax
from jax.experimental import pallas as pl
from jax.experimental.pallas import tpu as pltpu
from jax.sharding import PartitionSpec as P

BAND = 12
HALO = 2 * BAND
CHUNKS = 4
hybrid_ens = 0.75
hybrid_static = 0.25
F32, BF16 = jnp.float32, jnp.bfloat16
HI = lax.Precision.HIGHEST
MESH = pl.DeviceIdType.MESH
AROUND = [(dx, dy) for dy in (0, 1, -1) for dx in (1, -1, 0) if (dx, dy) != (0, 0)]


def iota(shape, axis):
    return lax.broadcasted_iota(jnp.int32, shape, axis)


def dot(a, b, precision=None):
    return jnp.dot(a, b, preferred_element_type=F32, precision=precision)


def split(x):
    high = x.astype(BF16)
    return high, (x - high.astype(F32)).astype(BF16)


def kernel(dims, band_any, a_any, s_any, idx_any, inn_any, wt_any, ens_out, static_out, lam_out,
           band_ref, idx_ref, inn_ref, wt_ref, ac, kl, kr, hl, hr, f0c, k0l, k0r, f0l, f0r, f1c, k1l, k1r, f1l, f1r,
           obs, mlat, nlon, nrim, xs, ub, us, p_ref, ps_ref, lam_ref, sl, y_ref, yr, t1_ref, gather_plane, gather_lon,
           in_sem, a_send, a_recv, f0_send, f0_recv, z_send, z_recv, f1_send, f1_recv, r0_send, r0_recv, r1_send, r1_recv,
           g_send, g_recv, c1_send, c1_recv, q0_send, q0_recv, q1_send, q1_recv, sp_send, sp_recv, so_send, so_recv, out_sem):
    n_lon, n_lat, n_mem, members, levels, rows, cols = dims
    lon, lat, mem = lax.axis_index("lon"), lax.axis_index("lat"), lax.axis_index("mem")
    ce2 = hybrid_ens / (members * n_mem)
    cs2 = hybrid_static
    ext = rows + 2 * HALO

    def at(dlon=0, dlat=0, dmem=0):
        return {
            "lon": lax.rem(lon + (dlon + n_lon), n_lon),
            "lat": lax.rem(lat + (dlat + n_lat), n_lat),
            "mem": lax.rem(mem + (dmem + n_mem), n_mem),
        }

    def copy(src, dst, send, recv, device):
        return pltpu.make_async_remote_copy(
            src_ref=src, dst_ref=dst, send_sem=send, recv_sem=recv, device_id=device, device_id_type=MESH
        )
    parity = lax.rem(lon, 2)
    across = 1 - 2 * parity
    plane = [(tx * across, ol, om) for tx in range(2) for ol in range(n_lat) for om in range(n_mem)][1:]
    line = [(o, 0, 0) for o in range(2, n_lon, 2)]
    partners = line + plane[::-1] + [(-across, dy, 0) for dy in (0, 1, -1)] + [(-across, 0, o) for o in range(1, n_mem)]
    barrier = pltpu.get_barrier_semaphore()
    for partner in partners:
        pl.semaphore_signal(barrier, inc=1, device_id=at(*partner), device_id_type=MESH)

    own = pl.ds(0, rows)
    inputs = [
        pltpu.make_async_copy(src, dst, in_sem.at[number])
        for number, (src, dst) in enumerate((
            (a_any, ac.at[:, :, own, :]), (s_any.at[mem], f0c.at[levels, own, :]), (band_any, band_ref),
            (idx_any, idx_ref), (inn_any, inn_ref), (wt_any, wt_ref),
        ))
    ]
    for one in inputs:
        one.start()
    low, high = pl.ds(rows, HALO), pl.ds(rows + HALO, HALO)
    first, last = pl.ds(0, HALO), pl.ds(rows - HALO, HALO)
    sel_row, sel_col = iota((levels * cols, 2 * cols), 0), iota((levels * cols, 2 * cols), 1)
    sel_level, sel_lat = sel_row // cols, lax.rem(sel_row, cols)
    spot = lax.rem(sel_col, cols) - HALO * sel_level
    wanted = jnp.where(sel_col < cols, spot + (cols - HALO), spot)
    select = jnp.where((spot >= 0) & (spot < HALO) & (sel_lat == wanted), 1.0, 0.0)

    for one in inputs:
        one.wait()
    packed = dot(
        jnp.concatenate([ac[:, l, own, :].reshape(members * rows, cols) for l in range(levels)], axis=1),
        select.astype(BF16),
    ).astype(BF16)
    kl[...] = packed[:, :cols].reshape(members, rows, cols)
    kr[...] = packed[:, cols:].reshape(members, rows, cols)
    pl.semaphore_wait(barrier, len(partners))

    from_rows = {1: last, -1: first, 0: pl.ds(0, rows)}
    to_rows = {1: low, -1: high, 0: own}

    def halo(centre, left, right, packed_left, packed_right, send, recv, chunk=None, takes=lambda dx, dy: True):
        copies = []
        for number, (dx, dy) in enumerate(AROUND):
            if not takes(dx, dy):
                continue
            if dy == 0:
                if chunk is None:
                    src, dst = centre.at[:, from_rows[dx], :], centre.at[:, to_rows[dx], :]
                else:
                    src, dst = centre.at[chunk, :, from_rows[dx], :], centre.at[chunk, :, to_rows[dx], :]
            else:
                every = slice(None) if chunk is None else chunk
                src = (packed_left if dy == 1 else packed_right).at[every, from_rows[dx], :]
                dst = (left if dy == 1 else right).at[every, to_rows[dx], :]
            one = copy(src, dst, send.at[number], recv.at[number], at(dx, dy))
            one.start()
            copies.append(one)
        return copies

    batch = members // CHUNKS

    def send_chunk(number):
        return halo(
            ac, hl, hr, kl, kr, a_send.at[number], a_recv.at[number], pl.ds(number * batch, batch),
            lambda dx, dy: dx != 0,
        )
    a_copies = [send_chunk(0)]
    a_lat = halo(
        ac, hl, hr, kl, kr, a_send.at[0], a_recv.at[0], pl.ds(0, members), lambda dx, dy: dx == 0
    )
    index = idx_ref[...]
    weight = wt_ref[...]
    at_row, at_col = index // cols, lax.rem(index, cols)
    count = index.shape[1]
    columns = jnp.where(iota((cols, count), 0) == at_col, 1.0, 0.0).astype(BF16)

    def thirds(v):
        one = v.astype(BF16).astype(F32)
        two = (v - one).astype(BF16).astype(F32)
        return [one, two, v - one - two]

    terms = thirds(weight) + thirds(weight * inn_ref[...])

    def level_fields(l, carry):
        here = (iota((rows, count), 0) + rows * l) == at_row
        stacked = jnp.concatenate([jnp.where(here, t, 0.0).astype(BF16) for t in terms], axis=0)
        sums = lax.dot_general(stacked, columns, (((1,), (1,)), ((), ())), preferred_element_type=F32)
        obs[l] = sums[0:rows] + sums[rows:2 * rows] + sums[2 * rows:3 * rows]
        f0c[l, own, :] = sums[3 * rows:4 * rows] + sums[4 * rows:5 * rows] + sums[5 * rows:]
        return carry

    lax.fori_loop(0, levels, level_fields, 0)

    select16 = select.astype(BF16)

    def select_exact(x, chosen):
        terms = dot(jnp.concatenate([t.astype(BF16) for t in thirds(x)], axis=0), chosen)
        return terms[0:rows] + terms[rows:2 * rows] + terms[2 * rows:]

    def pack(centre, left, right, extra=0.0):
        whole = jnp.concatenate([centre[l, own, :] for l in range(levels)], axis=1)
        both = select_exact(whole, select16) + extra
        left[0] = both[:, :cols]
        right[0] = both[:, cols:]

    spare = levels * HALO
    spot = lax.rem(iota((cols, 2 * cols), 1), cols) - spare
    wanted = jnp.where(iota((cols, 2 * cols), 1) < cols, spot + (cols - HALO), spot)
    place = jnp.where((spot >= 0) & (spot < HALO) & (iota((cols, 2 * cols), 0) == wanted), 1.0, 0.0)
    pack(f0c, k0l, k0r, select_exact(f0c[levels, own, :], place.astype(BF16)))
    half = levels // 2
    ours = pl.ds(half * lax.rem(mem, 2), half)
    twin = 1 - 2 * lax.rem(mem, 2)
    z_copies, s_copies = [], []
    for number, dx in enumerate((1, -1)):
        for kind, (some, group) in enumerate(((ours, z_copies), (pl.ds(levels, 1), s_copies))):
            one = copy(
                f0c.at[some, from_rows[dx], :], f0c.at[some, to_rows[dx], :],
                z_send.at[2 * kind + number], z_recv.at[2 * kind + number], at(dx, 0, 0),
            )
            one.start()
            group.append(one)
    f0_lat = halo(f0c, f0l, f0r, k0l, k0r, f0_send, f0_recv, takes=lambda dx, dy: dx == 0)
    f0_copies = s_copies + halo(
        f0c, f0l, f0r, k0l, k0r, f0_send, f0_recv, takes=lambda dx, dy: dx != 0 and dy != 0
    )
    a_copies.append(send_chunk(1))
    r, c = iota((cols, cols), 0), iota((cols, cols), 1)
    inside_low = jnp.where(lat > 0, 1.0, 0.0).astype(F32)
    inside_high = jnp.where(lat < n_lat - 1, 1.0, 0.0).astype(F32)
    offsets = iota((8, cols), 1) - BAND

    def spot_of(row):
        return jnp.where(row < rows, row, jnp.where(row < rows + HALO, row - rows - HALO, row - HALO))

    def level_matrices(l, carry):
        def band_of(which):
            width = jnp.full((1, 1), band_ref[which, l].astype(F32), F32)

            def raw(diff):
                d = diff.astype(F32)
                ratio = d / (0.5 * width)
                return jnp.where(jnp.abs(d) <= width, jnp.exp(-0.5 * (ratio * ratio)), 0.0)

            total = jnp.sum(raw(offsets), axis=1, keepdims=True)[0:1]
            return lambda diff: raw(diff) / total

        band = band_of(1)
        spot = r - HALO * l
        valid = jnp.where((spot >= 0) & (spot < HALO), 1.0, 0.0)
        d0, dm, dp = band(r - c), band(r - cols - c), band(r + cols - c)
        from_low = spot + (cols - HALO)
        dml, d0l = band(from_low - cols - c) * valid, band(from_low - c) * valid
        dpr, d0r = band(spot + cols - c) * valid, band(spot - c) * valid
        twice = [
            dot(d0, d0, HI) + inside_low * dot(dp, dm, HI) + inside_high * dot(dm, dp, HI),
            inside_low * (dot(d0l, dm, HI) + dot(dml, d0, HI)),
            inside_high * (dot(d0r, dp, HI) + dot(dpr, d0, HI)),
        ]
        once = [d0, inside_low * dml, inside_high * dpr]
        for part in range(3):
            hi, lo = split(jnp.concatenate([twice[part], once[part]], axis=1))
            mlat[l, part * cols:(part + 1) * cols, :] = hi
            mlat[l, (3 + part) * cols:(4 + part) * cols, :] = hi
            mlat[l, (6 + part) * cols:(7 + part) * cols, :] = lo
        band = band_of(0)
        near = band(iota((rows, ext), 0) - spot_of(iota((rows, ext), 1)))
        far = band(spot_of(iota((ext, ext), 0)) - spot_of(iota((ext, ext), 1)))
        for which, matrix in enumerate((dot(near, far, HI), near)):
            hi, lo = split(matrix)
            nlon[which, l, 0:rows, :] = hi
            nlon[which, l, rows:2 * rows, :] = lo
            nrim[which, l, 0:rows, :] = hi[:, rows:]
            nrim[which, l, rows:2 * rows, :] = lo[:, rows:]
        return carry

    lax.fori_loop(0, levels, level_matrices, 0)
    a_copies.append(send_chunk(2))
    def lon_pass(l, u_hi, u_lo, which, matrix=nlon):
        depth = u_hi.shape[0]
        both = matrix[which, l] if matrix.shape[3] == depth else matrix[which, l, :, 0:depth]
        tall = dot(both, u_hi)
        return tall[0:rows] + tall[rows:] + dot(both[0:rows], u_lo)

    own_rows, rim_rows = (0, rows, 0), (rows, 2 * HALO, members * rows)

    def apply_members(centre, left, right, start, count, part, fresh):
        row, size, base = part
        some = pl.ds(row, size)
        zl, zr = left[0, some, :], right[0, some, :]
        z = [centre[l, some, :] for l in range(levels)]
        chunk = pl.ds(base + start * size, count * size)
        for k in range(start, start + count):
            spans = pl.ds(base + k * size, size)
            for side, (rim, zz) in enumerate(((hl, zl), (hr, zr))):
                hi, lo = split(rim[k, some, :].astype(F32) * zz)
                for l in range(levels):
                    xs[l, spans, (1 + side) * cols:(2 + side) * cols] = hi
                    xs[l, spans, (4 + side) * cols:(5 + side) * cols] = lo
            for l in range(levels):
                hi, lo = split(ac[k, l, some, :].astype(F32) * z[l])
                xs[l, spans, 0:cols] = hi
                xs[l, spans, 3 * cols:4 * cols] = lo
        for l in range(levels):
            ub[l, chunk, :] = dot(xs[l, chunk, :], mlat[l, 0:6 * cols, :]) + dot(
                xs[l, chunk, 0:3 * cols], mlat[l, 6 * cols:, :]
            )
        for l in range(levels):
            total = jnp.zeros((rows, cols), F32)
            for k in range(start, start + count):
                hi, lo = split(ub[l, pl.ds(base + k * size, size), 0:cols])
                part_sum = lon_pass(l, hi, lo, 0, nrim if row else nlon)
                total += ac[k, l, own, :].astype(F32) * part_sum
            y_ref[l] = ce2 * total if fresh else y_ref[l] + ce2 * total

    def apply_static(centre, left, right):
        his, los = [], []
        for stat, z in ((f0c[levels], centre[mem]), (sl[0], left[0]), (sl[1], right[0])):
            hi, lo = split(stat * z)
            his.append(hi)
            los.append(lo)
        u = dot(jnp.concatenate(his + los, axis=1), mlat[mem, 0:6 * cols, :])
        us[...] = u + dot(jnp.concatenate(his, axis=1), mlat[mem, 6 * cols:, :])
        hi, lo = split(us[:, 0:cols])
        y_ref[mem] = y_ref[mem] + cs2 * f0c[levels, own, :] * lon_pass(mem, hi, lo, 0)

    def parts(turn, which):
        for l in which:
            for k in range(members):
                u = jnp.concatenate(
                    [ub[l, pl.ds(base + k * size, size), cols:2 * cols] for _, size, base in (own_rows, rim_rows)],
                    axis=0,
                )
                hi, lo = split(u)
                p_ref[turn, k, l] = math.sqrt(ce2) * lon_pass(l, hi, lo, 1)

    def static_part(turn, send, recv):
        hi, lo = split(us[:, cols:2 * cols])
        ps_ref[turn, mem] = math.sqrt(cs2) * lon_pass(mem, hi, lo, 1)
        copies = []
        for o in range(1, n_mem):
            one = copy(
                ps_ref.at[turn, mem], ps_ref.at[turn, mem], send.at[o - 1], recv.at[o - 1], at(0, 0, o)
            )
            one.start()
            copies.append(one)
        return copies

    def scatter_sum(slots, send, recv):
        copies = []
        for o in range(1, n_mem):
            other = lax.rem(mem + o, n_mem)
            one = copy(y_ref.at[other], slots.at[o - 1], send.at[o - 1], recv.at[o - 1], at(0, 0, o))
            one.start()
            copies.append(one)
        return copies

    def finish_sum(copies, slots):
        total = y_ref[mem]
        for o, one in enumerate(copies):
            one.wait()
            total = total + slots[o]
        return total

    for one in a_lat + f0_lat:
        one.wait_recv()
    apply_members(f0c, f0l, f0r, 0, members, own_rows, True)
    for number, (one, rim) in enumerate(zip(z_copies, (low, high))):
        one.wait_recv()
        passed = copy(
            f0c.at[ours, rim, :], f0c.at[ours, rim, :],
            z_send.at[4 + number], z_recv.at[4 + number], at(0, 0, twin),
        )
        passed.start()
        f0_copies.append(passed)
    a_copies.append(send_chunk(3))
    for one in f0_copies:
        one.wait_recv()
    realign = jnp.where((r - spare == c - HALO * mem) & (r >= spare) & (r < spare + HALO), 1.0, 0.0)
    sl[0] = dot(f0l[0], realign, HI)
    sl[1] = dot(f0r[0], realign, HI)

    for number in range(CHUNKS):
        for one in a_copies[number]:
            one.wait_recv()
        apply_members(f0c, f0l, f0r, number * batch, batch, rim_rows, False)
    r0_copies = scatter_sum(yr.at[0], r0_send, r0_recv)
    apply_static(f0c, f0l, f0r)
    parts(0, (0, 1))
    y0 = finish_sum(r0_copies, yr.at[0])
    t0 = f0c[mem, own, :]
    t1 = obs[mem] * y0
    t1_ref[...] = t1
    f1c[mem, own, :] = t1
    g_copies, c1_copies = [], []
    for o in range(1, n_mem):
        one = copy(t1_ref, f1c.at[mem, own, :], g_send.at[o - 1], g_recv.at[o - 1], at(0, 0, o))
        one.start()
        g_copies.append(one)
    parts(0, (2, 3))
    outs = [pltpu.make_async_copy(p_ref.at[0], ens_out.at[0], out_sem.at[0])]
    outs[-1].start()
    for one in g_copies:
        one.wait_recv()
    pack(f1c, k1l, k1r)
    f1_lat = halo(f1c, f1l, f1r, k1l, k1r, f1_send, f1_recv, takes=lambda dx, dy: dx == 0)
    f1_corners = halo(f1c, f1l, f1r, k1l, k1r, f1_send, f1_recv, takes=lambda dx, dy: dx != 0 and dy != 0)
    for number, dx in enumerate((1, -1)):
        for o in range(n_mem):
            one = copy(
                t1_ref.at[from_rows[dx], :], f1c.at[mem, to_rows[dx], :],
                c1_send.at[number, o], c1_recv.at[number, o], at(dx, 0, o),
            )
            one.start()
            c1_copies.append(one)
    for one in f1_lat:
        one.wait_recv()
    apply_members(f1c, f1l, f1r, 0, members, own_rows, True)
    for one in f1_corners + c1_copies:
        one.wait_recv()
    q0_copies = static_part(0, q0_send, q0_recv)
    apply_members(f1c, f1l, f1r, 0, members, rim_rows, False)
    r1_copies = scatter_sum(yr.at[1], r1_send, r1_recv)
    apply_static(f1c, f1l, f1r)
    parts(1, range(levels))
    outs.append(pltpu.make_async_copy(p_ref.at[1], ens_out.at[1], out_sem.at[1]))
    outs[-1].start()
    y1 = finish_sum(r1_copies, yr.at[1])

    def summed(x):
        return jnp.sum(jnp.sum(x, axis=0, keepdims=True), axis=1, keepdims=True)

    lane = iota((8, cols), 1)
    sums = jnp.zeros((8, cols), F32)
    for number, value in enumerate((t0 * y0, t1 * y0, t1 * y1, y1 * (obs[mem] * y1))):
        sums = jnp.where(lane == number, summed(value), sums)

    def total_start(value, slots, me, offsets, send, recv):
        slots[me] = value
        copies = []
        for number, offset in enumerate(offsets):
            one = copy(slots.at[me, 0:1, :], slots.at[me, 0:1, :], send.at[number], recv.at[number], at(*offset))
            one.start()
            copies.append(one)
        return copies

    def total_finish(slots, copies):
        for one in copies:
            one.wait_recv()
        out = slots[0, 0:1, :]
        for other in range(1, len(copies) + 1):
            out = out + slots[other, 0:1, :]
        return jnp.broadcast_to(out, (8, cols))

    plane_copies = total_start(sums, gather_plane, (parity * n_lat + lat) * n_mem + mem, plane, sp_send, sp_recv)
    sums = total_finish(gather_plane, plane_copies)
    line_copies = total_start(sums, gather_lon, lon // 2, line, so_send, so_recv)
    q1_copies = static_part(1, q1_send, q1_recv)
    for one in q0_copies + q1_copies:
        one.wait()
    outs.append(pltpu.make_async_copy(ps_ref, static_out, out_sem.at[3]))
    outs[-1].start()
    sums = total_finish(gather_lon, line_copies)
    row = sums[0:1]

    def pick(number):
        return jnp.sum(jnp.where(iota((1, cols), 1) == number, row, 0.0), axis=1, keepdims=True)

    rr = pick(0)
    u, v, s = pick(1) / rr, pick(2) / rr, pick(3) / rr
    alpha = 1.0 / (1.0 + u)
    beta = (v - u * u) * alpha * alpha
    g, h = 1.0 - alpha + beta, -alpha
    alpha_next = beta / (g * g * (1.0 + u) + 2.0 * g * h * (u + v) + h * h * (v + s))
    lam_ref[...] = jnp.where(lane == 0, alpha + alpha_next * g, alpha_next * h)
    outs.append(pltpu.make_async_copy(lam_ref, lam_out, out_sem.at[2]))
    outs[-1].start()
    for one in outs:
        one.wait()
    for copies in a_copies:
        for one in copies:
            one.wait_send()
    for one in z_copies + f0_lat + f0_copies + g_copies + c1_copies + f1_lat + f1_corners + a_lat + plane_copies + line_copies:
        one.wait_send()


def combine(ens_in, static_in, lam_in, ens_out, static_out, ens, static, lam, ens_sem, in_sem, out_sem):
    members = ens_out.shape[0]
    lam_copy = pltpu.make_async_copy(lam_in, lam, in_sem.at[0])
    static_copy = pltpu.make_async_copy(static_in, static, in_sem.at[1])
    lam_copy.start()
    loads = [pltpu.make_async_copy(ens_in.at[:, k], ens.at[:, k], ens_sem.at[k]) for k in range(members)]
    for one in loads:
        one.start()
    static_copy.start()
    lam_copy.wait()
    near, far = lam[0:1, 0:1], lam[0:1, 1:2]
    stores = []
    for k in range(members):
        loads[k].wait()
        ens[0, k] = near * ens[0, k] + far * ens[1, k]
        stores.append(pltpu.make_async_copy(ens.at[0, k], ens_out.at[k], out_sem.at[k]))
        stores[-1].start()
    static_copy.wait()
    static[0] = near * static[0] + far * static[1]
    stores.append(pltpu.make_async_copy(static.at[0], static_out, out_sem.at[members]))
    stores[-1].start()
    for one in stores:
        one.wait()


def per_device(n_lon, n_lat, n_mem, anomalies, spread, obs_index, innovation, obs_weight, band_width):
    members, levels, rows, cols = anomalies.shape
    ext = rows + 2 * HALO
    count = obs_index.shape[-1]
    vmem, dma = pltpu.VMEM, pltpu.SemaphoreType.DMA
    dims = (n_lon, n_lat, n_mem, members, levels, rows, cols)
    far = pl.BlockSpec(memory_space=pltpu.HBM)
    done = pl.pallas_call(
        lambda *refs: kernel(dims, *refs),
        out_shape=(
            jax.ShapeDtypeStruct((2, members, levels, rows, cols), F32),
            jax.ShapeDtypeStruct((2, levels, rows, cols), F32),
            jax.ShapeDtypeStruct((8, cols), F32),
        ),
        in_specs=[far] * 6,
        out_specs=(far, far, far),
        scratch_shapes=[
            pltpu.SMEM((2, levels), jnp.int32),
            vmem((1, count), jnp.int32), vmem((1, count), F32), vmem((1, count), F32),
            vmem((members, levels, ext, cols), BF16),
            vmem((members, rows, cols), BF16), vmem((members, rows, cols), BF16),
            vmem((members, ext, cols), BF16), vmem((members, ext, cols), BF16),
            vmem((levels + 1, ext, cols), F32),
            vmem((1, rows, cols), F32), vmem((1, rows, cols), F32),
            vmem((1, ext, cols), F32), vmem((1, ext, cols), F32),
            vmem((levels, ext, cols), F32),
            vmem((1, rows, cols), F32), vmem((1, rows, cols), F32),
            vmem((1, ext, cols), F32), vmem((1, ext, cols), F32),
            vmem((levels, rows, cols), F32),
            vmem((levels, 9 * cols, 2 * cols), BF16),
            vmem((2, levels, 2 * rows, ext), BF16),
            vmem((2, levels, 2 * rows, 2 * HALO), BF16),
            vmem((levels, members * ext, 6 * cols), BF16),
            vmem((levels, members * ext, 2 * cols), F32),
            vmem((ext, 2 * cols), F32),
            vmem((2, members, levels, rows, cols), F32),
            vmem((2, levels, rows, cols), F32),
            vmem((8, cols), F32),
            vmem((2, ext, cols), F32),
            vmem((levels, rows, cols), F32),
            vmem((2, n_mem - 1, rows, cols), F32),
            vmem((rows, cols), F32),
            vmem((2 * n_lat * n_mem, 8, cols), F32), vmem((n_lon // 2, 8, cols), F32),
        ]
        + [dma((6,))]
        + [dma((CHUNKS, 8))] * 2
        + [dma((8,))] * 2
        + [dma((6,))] * 2
        + [dma((8,))] * 2
        + [dma((n_mem - 1,))] * 4
        + [dma((n_mem - 1,))] * 2
        + [dma((2, n_mem))] * 2
        + [dma((n_mem - 1,))] * 4
        + [dma((2 * n_lat * n_mem - 1,))] * 2
        + [dma((n_lon // 2 - 1,))] * 2
        + [dma((4,))],
        compiler_params=pltpu.CompilerParams(
            collective_id=0, has_side_effects=True, vmem_limit_bytes=63 * 1024 * 1024
        ),
    )(
        band_width, anomalies, spread, obs_index.reshape(1, count), innovation.reshape(1, count),
        obs_weight.reshape(1, count),
    )
    return pl.pallas_call(
        combine,
        out_shape=(
            jax.ShapeDtypeStruct((members, levels, rows, cols), F32),
            jax.ShapeDtypeStruct((levels, rows, cols), F32),
        ),
        in_specs=[far] * 3,
        out_specs=(far, far),
        scratch_shapes=[
            vmem((2, members, levels, rows, cols), F32), vmem((2, levels, rows, cols), F32), vmem((8, cols), F32),
            dma((members,)), dma((2,)), dma((members + 1,)),
        ],
        compiler_params=pltpu.CompilerParams(vmem_limit_bytes=63 * 1024 * 1024),
    )(*done)


def solution(mesh):
    n_lon, n_lat, n_mem = (mesh.shape[name] for name in ("lon", "lat", "mem"))
    return jax.shard_map(
        lambda *args: per_device(n_lon, n_lat, n_mem, *args),
        mesh=mesh,
        in_specs=(
            P("mem", None, "lon", "lat"),
            P(None, "lon", "lat"),
            P("lon", "lat", None),
            P("lon", "lat", None),
            P("lon", "lat", None),
            P(),
        ),
        out_specs=(P("mem", None, "lon", "lat"), P(None, "lon", "lat")),
        check_vma=False,
    )
```
